32 devices in a mesh: parts: 1, seq: 8 (over z, y), head: 2 (over x), rep: 2 (over core).
Axes of the slice: x: 2, y: 2, z: 4, core: 2. Of those that a mesh axis runs over, the one named last changes fastest.
Arguments:
- residual: bfloat16 [16, 8192], P(('parts', 'head'), ('seq', 'rep')), may hold values from -48 to 48
- coefficients: float32 [16, 16], P(('parts', 'head')), may hold values from -6 to 6
- directions: float32 [16, 8192], P(None, ('seq', 'rep')), may hold values from -1.5 to 1.5
- attn_gain: float32 [8192], P(('seq', 'rep')), may hold values from 0.25 to 1.75
- mlp_gain: float32 [8192], replicated, may hold values from 0.25 to 1.75
- w_query: bfloat16 [8192, 8192], P(('seq', 'rep'), 'head'), may hold values from -0.0625 to 0.0625
- w_output: bfloat16 [8192, 8192], P('head', ('seq', 'rep')), may hold values from -0.0625 to 0.0625
- w_gate: bfloat16 [8192, 14336], P('head', ('seq', 'rep')), may hold values from -0.0625 to 0.0625
- w_up: bfloat16 [8192, 14336], P('head', ('seq', 'rep')), may hold values from -0.0625 to 0.0625
- w_down: bfloat16 [14336, 8192], P(('seq', 'rep'), 'head'), may hold values from -0.046875 to 0.046875
- prefix_keys: bfloat16 [8192, 8, 128], P(('parts', 'seq', 'rep'), 'head'), may hold values from -500 to 500
- prompt_value_rows: bfloat16 [8192, 8, 128], P(('parts', 'seq', 'rep'), 'head'), may hold values from -6 to 6
- private_suffix_keys: bfloat16 [16, 128, 8, 128], P(('parts', 'seq', 'rep'), None, 'head'), may hold values from -21 to 21
- private_suffix_values: bfloat16 [16, 128, 8, 128], P(('parts', 'seq', 'rep'), None, 'head'), may hold values from -6 to 6
- suffix_lengths: int32 [16], P('parts'), may hold values from 1 to 128, 1024 in all
Outputs:
- mixed: bfloat16 [16, 8192], P(('parts', 'seq', 'rep'), 'head')
The draws below stay inside these ranges and needn't reach their ends.
Inputs may be any that keep to these rules, and one draw needn't show every extreme that they name: Row r's suffix holds suffix_lengths[r] live tokens in its first slots; the lengths sum to 1024 and the largest is exactly 128.
All inputs are finite; a program needn't handle non-finite values.
Results may differ from the reference program's by a relative error of at most 0.024.
Values may be sent and summed in bfloat16 or wider, within the bound.
No kernel may reach another device: no remote copies, remote signals or barrier semaphores. Data moves between devices by JAX's collectives and lax.ppermute only.
A program may use at most 64 MiB of HBM per device.

```python
import math
import jax
import jax.numpy as jnp
import numpy as np
from jax import lax

D = 8192
QUERY_HEADS = 64
KEY_VALUE_HEADS = 8
HEAD_SIZE = 128
FF = 14336
NDIR = 16
SUFFIX_TOKENS = 128
QW = 8192
BRANCH_ROWS = 16
PROMPT_TOKENS = 8192


def draw_residual(key, part):
    key_rows = jax.random.split(key, 3)
    row_scale = jnp.exp(jax.random.uniform(key_rows[1], (BRANCH_ROWS, 1), jnp.float32, math.log(0.4), math.log(4.0)))
    rough_factor = jnp.exp(jax.random.uniform(key_rows[2], (1, D), jnp.float32, math.log(0.6), math.log(1.6)))
    column_place = jnp.arange(D, dtype=jnp.float32)[None, :] / float(D - 1)
    slope_scale = jnp.exp(math.log(3.0) - math.log(6.0) * column_place)
    values = jax.random.normal(key_rows[0], (BRANCH_ROWS, D), jnp.float32)
    return jnp.clip(values * row_scale * rough_factor * slope_scale, -48.0, 48.0).astype(jnp.bfloat16)


def draw_prefix_keys(key, part):
    key_rows = jax.random.split(key, 1)
    array_shape = (PROMPT_TOKENS, KEY_VALUE_HEADS, HEAD_SIZE)
    values = 2.5 * jnp.clip(jax.random.normal(key_rows[0], array_shape, jnp.float32), -6.0, 6.0)
    return jnp.clip(values, -500.0, 500.0).astype(jnp.bfloat16)


def level_of(key, extent, shards, smallest, high):
    loudness, own = 1.0, jax.random.fold_in(key, 6)
    for position, shards_of in shards:
        steps = jnp.exp(jax.random.uniform(jax.random.fold_in(own, position), (shards_of,), jnp.float32, smallest / len(shards), high / len(shards)))
        loudness = loudness * jnp.repeat(steps, extent[position] // shards_of).reshape([-1 if axis == position else 1 for axis in range(len(extent))])
    return loudness


def length_profile(number_of, total, bound, skew):
    portions = [(1 << 20) // math.isqrt(standing ** skew) + 1 for standing in range(2, number_of + 1)]
    rest, counts = total - bound - (number_of - 1), [1] * (number_of - 1)
    while rest > 0:
        movable = [i for i in range(number_of - 1) if counts[i] < bound]
        whole, left = sum([portions[i] for i in movable]), rest
        for i in movable:
            extra = min(bound - counts[i], max(1, left * portions[i] // whole), rest)
            counts[i] = counts[i] + extra
            rest = rest - extra
    return np.array([bound] + counts)


def ragged_sizes(key, number_of, total, reach, lean):
    if number_of == 2:
        one = jax.random.randint(key, (), max(1, total - reach), min(reach, total - 1) + 1)
        return jnp.stack([one, total - one])
    tallies = jnp.asarray(length_profile(number_of, total, reach, lean), jnp.int32)
    pairs = (number_of - 1) // 2
    source_of, taker = tallies[1:1 + 2 * pairs:2], tallies[2:2 + 2 * pairs:2]
    margin = jnp.minimum(source_of - 1, reach - taker)
    shifted = jax.random.randint(jax.random.fold_in(key, 1), (pairs,), 0, 1 << 20) % (margin + 1)
    tallies = tallies.at[1:1 + 2 * pairs:2].set(source_of - shifted).at[2:2 + 2 * pairs:2].set(taker + shifted)
    return tallies[jax.random.permutation(jax.random.fold_in(key, 2), number_of)]


def noise(own_key, extent, width, reach, cuts=(), held_as=jnp.bfloat16):
    entries = jax.random.normal(own_key, extent, jnp.float32) * width
    if len(cuts) > 0:
        entries = level_of(own_key, extent, cuts, -0.22, 0.18) * entries
    return jnp.clip(entries, min=-reach, max=reach).astype(held_as)


def setup_inputs(seed: int = 0, part: int = 0) -> dict:
    seeds = jax.random.split(jax.random.key(seed), 16)
    part_keys = jax.random.split(jax.random.fold_in(seeds[15], part), 16)
    residual = draw_residual(jax.random.fold_in(jax.random.fold_in(seeds[15], part), 71), part)
    coefficients = noise(part_keys[1], (BRANCH_ROWS, NDIR), 1.0, 6.0, ((0, 2),), jnp.float32)
    directions = noise(seeds[2], (NDIR, D), 0.25, 1.5, ((1, 16),), jnp.float32)
    attn_gain = jnp.clip(1.0 + 0.15 * jax.random.normal(seeds[3], (D,), jnp.float32), 0.25, 1.75)
    mlp_gain = jnp.clip(1.0 + 0.15 * jax.random.normal(seeds[4], (D,), jnp.float32), 0.25, 1.75)
    w_query = noise(seeds[5], (D, QW), D ** -0.5, 0.0625, ((0, 16), (1, 2)))
    w_output = noise(seeds[6], (QW, D), QW ** -0.5, 0.0625, ((0, 2), (1, 16)))
    w_gate = noise(seeds[7], (D, FF), D ** -0.5, 0.0625, ((0, 2), (1, 16)))
    w_up = noise(seeds[8], (D, FF), D ** -0.5, 0.0625, ((0, 2), (1, 16)))
    w_down = noise(seeds[9], (FF, D), FF ** -0.5, 0.046875, ((0, 16), (1, 2)))
    prefix_keys = draw_prefix_keys(jax.random.fold_in(jax.random.fold_in(seeds[15], part), 71), part)
    prompt_value_rows = noise(part_keys[11], (PROMPT_TOKENS, KEY_VALUE_HEADS, HEAD_SIZE), 1.0, 6.0, ((0, 16), (1, 2)))
    private_suffix_keys = noise(part_keys[12], (BRANCH_ROWS, SUFFIX_TOKENS, KEY_VALUE_HEADS, HEAD_SIZE), 3.5, 21.0, ((0, 16), (2, 2)))
    private_suffix_values = noise(part_keys[13], (BRANCH_ROWS, SUFFIX_TOKENS, KEY_VALUE_HEADS, HEAD_SIZE), 1.0, 6.0, ((0, 16), (2, 2)))
    suffix_lengths = ragged_sizes(part_keys[14], BRANCH_ROWS, BRANCH_ROWS * SUFFIX_TOKENS // 2, SUFFIX_TOKENS, 2).astype(jnp.int32)
    return dict(residual=residual, coefficients=coefficients, directions=directions, attn_gain=attn_gain, mlp_gain=mlp_gain, w_query=w_query, w_output=w_output, w_gate=w_gate, w_up=w_up, w_down=w_down, prefix_keys=prefix_keys, prompt_value_rows=prompt_value_rows, private_suffix_keys=private_suffix_keys, private_suffix_values=private_suffix_values, suffix_lengths=suffix_lengths)


EPSILON = 1e-05
ROPE_BASE = 500000.0

def rotate(query_matrix, positions):
    half_width = query_matrix.shape[-1] // 2
    exponent = jnp.arange(half_width, dtype=jnp.float32) * (2.0 / query_matrix.shape[-1])
    frequency = jnp.exp(-math.log(ROPE_BASE) * exponent)
    angles = positions.astype(jnp.float32)[:, None] * frequency[None, :]
    cosine = jnp.cos(angles)[:, None, :]
    sine_part = jnp.sin(angles)[:, None, :]
    leading = query_matrix[..., :half_width]
    trailing = query_matrix[..., half_width:]
    return jnp.concatenate([leading * cosine - trailing * sine_part, trailing * cosine + leading * sine_part], axis=-1)

def reference(residual, coefficients, directions, attn_gain, mlp_gain, w_query, w_output, w_gate, w_up, w_down, prefix_keys, prompt_value_rows, private_suffix_keys, private_suffix_values, suffix_lengths):
    steered = residual.astype(jnp.float32) + jnp.dot(coefficients, directions, precision=lax.Precision.HIGHEST)
    inverse = lax.rsqrt(lax.optimization_barrier(jnp.sum(steered * steered, axis=1, keepdims=True)) / D + EPSILON)
    normed = (steered * inverse * attn_gain[None, :]).astype(jnp.bfloat16)
    raw_queries = jnp.dot(normed, w_query, preferred_element_type=jnp.float32)
    row_length_total = raw_queries.shape[0]
    positions = PROMPT_TOKENS + suffix_lengths - 1
    query_matrix = rotate(raw_queries.reshape(row_length_total, QUERY_HEADS, HEAD_SIZE), positions).astype(jnp.bfloat16)
    heads_per_group = QUERY_HEADS // KEY_VALUE_HEADS
    query_grouped = jnp.transpose(query_matrix.reshape(row_length_total, KEY_VALUE_HEADS, heads_per_group, HEAD_SIZE), (1, 0, 2, 3))
    score_scale = 1.0 / math.sqrt(HEAD_SIZE)
    live_mask = (jnp.arange(SUFFIX_TOKENS, dtype=jnp.int32)[None, :] < suffix_lengths[:, None])[:, None, :]

    def one_head(operands):
        head_queries, head_keys, head_values, tail_keys, tail_values = operands
        query_float = head_queries.astype(jnp.float32)
        prefix_scores = jnp.einsum('rgd,pd->rgp', query_float, head_keys.astype(jnp.float32)) * score_scale
        suffix_scores = jnp.einsum('rgd,rsd->rgs', query_float, tail_keys.astype(jnp.float32)) * score_scale
        suffix_scores = jnp.where(live_mask, suffix_scores, -jnp.inf)
        highest = jnp.maximum(lax.optimization_barrier(jnp.max(prefix_scores, axis=2)), lax.optimization_barrier(jnp.max(suffix_scores, axis=2)))[..., None]
        prefix_weights = jnp.exp(prefix_scores - highest)
        suffix_weights = jnp.where(live_mask, jnp.exp(suffix_scores - highest), 0.0)
        totals = lax.optimization_barrier(jnp.sum(prefix_weights, axis=2)) + lax.optimization_barrier(jnp.sum(suffix_weights, axis=2))
        prefix_rounded = lax.optimization_barrier(prefix_weights.astype(jnp.bfloat16)).astype(jnp.float32)
        suffix_rounded = lax.optimization_barrier(suffix_weights.astype(jnp.bfloat16)).astype(jnp.float32)
        weighted = jnp.einsum('rgp,pd->rgd', prefix_rounded, head_values.astype(jnp.float32))
        weighted = weighted + jnp.einsum('rgs,rsd->rgd', suffix_rounded, tail_values.astype(jnp.float32))
        return (weighted / totals[..., None]).astype(jnp.bfloat16)
    operands = (query_grouped, jnp.transpose(prefix_keys, (1, 0, 2)), jnp.transpose(prompt_value_rows, (1, 0, 2)), jnp.transpose(private_suffix_keys, (2, 0, 1, 3)), jnp.transpose(private_suffix_values, (2, 0, 1, 3)))
    attended = jnp.transpose(lax.map(one_head, operands), (1, 0, 2, 3)).reshape(row_length_total, QUERY_HEADS * HEAD_SIZE)
    middle = (steered + jnp.dot(attended, w_output, preferred_element_type=jnp.float32)).astype(jnp.bfloat16)
    middle_float = lax.optimization_barrier(middle).astype(jnp.float32)
    inverse_mlp = lax.rsqrt(lax.optimization_barrier(jnp.sum(middle_float * middle_float, axis=1, keepdims=True)) / D + EPSILON)
    normed_mlp = (middle_float * inverse_mlp * mlp_gain[None, :]).astype(jnp.bfloat16)
    gate_out = jnp.dot(normed_mlp, w_gate, preferred_element_type=jnp.float32)
    up_out = jnp.dot(normed_mlp, w_up, preferred_element_type=jnp.float32)
    hidden = (jax.nn.silu(gate_out) * up_out).astype(jnp.bfloat16)
    return (middle_float + jnp.dot(hidden, w_down, preferred_element_type=jnp.float32)).astype(jnp.bfloat16)
```

```python
import functools
import math

import jax
import jax.numpy as jnp
from jax import lax
from jax.experimental import pallas as pl
from jax.experimental.pallas import tpu as pltpu
from jax.sharding import PartitionSpec as P

QUERY_HEADS = 64
KEY_VALUE_HEADS = 8
EPSILON = 1e-05
ROPE_BASE = 500000.0
LANES = ("seq", "rep")
F32 = jnp.float32
BF16 = jnp.bfloat16


def swap(x, axis, bit):
    size = lax.axis_size(axis)
    return lax.ppermute(x, axis, [(i, i ^ bit) for i in range(size)])


def bits_of(size):
    bit = 1
    while bit < size:
        yield bit
        bit *= 2


def take(x, start, size, axis):
    return lax.dynamic_slice_in_dim(x, start, size, axis)


def in_order(flag, mine, other, axis):
    first = jnp.where(flag, other, mine)
    second = jnp.where(flag, mine, other)
    return jnp.concatenate([first, second], axis=axis)


def split_parts(value, count):
    parts = []
    for _ in range(count):
        head = lax.reduce_precision(value, 8, 7)
        parts.append(head)
        value = value - head
    return parts


def local_call(body, outs, *args, flops=6_000_000_000):
    return pl.pallas_call(
        body,
        out_shape=outs,
        cost_estimate=pl.CostEstimate(flops=flops, bytes_accessed=1 << 20, transcendentals=0),
        compiler_params=pltpu.CompilerParams(vmem_limit_bytes=4 << 20),
    )(*args)


def add_kernel(total_ref, got_ref, next_ref, send_ref):
    total = total_ref[...] + got_ref[...].astype(F32)
    next_ref[...] = total
    send_ref[...] = total.astype(BF16)


def add_stage(total, got):
    return local_call(
        add_kernel,
        (jax.ShapeDtypeStruct(total.shape, F32), jax.ShapeDtypeStruct(total.shape, BF16)),
        total,
        got,
    )


def parts_of(value, heads):
    lane = lax.broadcasted_iota(jnp.int32, value.shape, 1)
    value = jnp.where(lane < heads, value, 0.0)
    packed = jnp.zeros_like(value)
    for i in range(3):
        head = value.astype(BF16).astype(F32)
        packed = packed + (pltpu.roll(head, i * heads, 1) if i else head)
        value = value - head
    return packed


def joined(packed, heads):
    lanes = packed.shape[1]
    value = packed
    for i in range(1, 3):
        value = value + pltpu.roll(packed, lanes - i * heads, 1)
    return value


def merge_kernel(heads, size, last, out_ref, lse_ref, got_ref, *refs):
    wide = heads * size
    own = lse_ref[...]
    other = joined(got_ref[:, wide:].astype(F32), heads)
    high = jnp.maximum(own, other)
    w_own = jnp.exp(own - high)
    w_other = jnp.exp(other - high)
    total = w_own + w_other
    share = w_own / total
    for h in range(heads):
        cols = slice(h * size, (h + 1) * size)
        theirs = got_ref[:, cols].astype(F32)
        merged = theirs + share[:, h : h + 1] * (out_ref[:, cols] - theirs)
        if last:
            refs[0][:, cols] = merged.astype(BF16)
        else:
            refs[0][:, cols] = merged
            refs[2][:, cols] = merged.astype(BF16)
    if not last:
        lse = high + jnp.log(total)
        refs[1][...] = lse
        refs[2][:, wide:] = parts_of(lse, heads).astype(BF16)


def merge_stage(state, got, heads, size, last):
    out, lse = state
    rows = out.shape[0]
    wide = heads * size
    if last:
        outs = jax.ShapeDtypeStruct((rows, wide), BF16)
    else:
        outs = (
            jax.ShapeDtypeStruct((rows, wide), F32),
            jax.ShapeDtypeStruct(lse.shape, F32),
            jax.ShapeDtypeStruct((rows, wide + lse.shape[1]), BF16),
        )
    return local_call(functools.partial(merge_kernel, heads, size, last), outs, out, lse, got)


def gather_head(x):
    if lax.axis_size("head") == 2:
        return in_order(lax.axis_index("head") == 1, x, swap(x, "head", 1), 0)
    return lax.all_gather(x, "head", axis=0, tiled=True)


def rope_tables(positions, width):
    half = width // 2
    exponent = jnp.arange(half, dtype=F32) * (2.0 / width)
    frequency = jnp.exp(-math.log(ROPE_BASE) * exponent)
    angles = positions.astype(F32)[:, None] * frequency[None, :]
    return jnp.cos(angles)[:, None, :], jnp.sin(angles)[:, None, :]


def rotate(queries, cosine, sine):
    half = queries.shape[-1] // 2
    lead, trail = queries[..., :half], queries[..., half:]
    return jnp.concatenate(
        [lead * cosine - trail * sine, trail * cosine + lead * sine], axis=-1
    )


def merge(one, two):
    out_one, lse_one = one
    out_two, lse_two = two
    high = jnp.maximum(lse_one, lse_two)
    w_one = jnp.exp(lse_one - high)
    w_two = jnp.exp(lse_two - high)
    total = w_one + w_two
    out = out_one * (w_one / total)[..., None] + out_two * (w_two / total)[..., None]
    return out, high + jnp.log(total)


def pack(out, lse):
    rows, heads, size = out.shape
    parts = jnp.concatenate(split_parts(lse, 3), axis=1)
    pad = -parts.shape[1] % 128
    parts = jnp.pad(parts, ((0, 0), (0, pad)))
    return jnp.concatenate([out.reshape(rows, heads * size), parts], axis=1).astype(BF16)


def unpack(sent, heads, size):
    rows = sent.shape[0]
    sent = sent.astype(F32)
    out = sent[:, : heads * size].reshape(rows, heads, size)
    parts = sent[:, heads * size : heads * (size + 3)].reshape(rows, 3, heads)
    return out, parts[:, 0] + parts[:, 1] + parts[:, 2]


def shards(
    residual,
    coefficients,
    directions,
    attn_gain,
    mlp_gain,
    w_query,
    w_output,
    w_gate,
    w_up,
    w_down,
    prefix_keys,
    prompt_value_rows,
    private_suffix_keys,
    private_suffix_values,
    suffix_lengths,
):
    lanes = lax.axis_size(LANES)
    lane = lax.axis_index(LANES)
    rep = lax.axis_index("rep")
    seq_size = lax.axis_size("seq")
    groups = lax.axis_size("head")
    group = lax.axis_index("head")
    block_rows = residual.shape[0]
    rows = block_rows * groups
    share = rows // lanes
    first_own = lane * share
    width = w_gate.shape[0] * groups
    prompt_length = prefix_keys.shape[0] * lanes
    kv_local, size = prefix_keys.shape[1:]
    heads_per_group = QUERY_HEADS // KEY_VALUE_HEADS
    heads = kv_local * heads_per_group
    suffix_tokens = private_suffix_keys.shape[1]

    steered = residual.astype(F32) + jnp.dot(
        coefficients, directions, precision=lax.Precision.HIGHEST
    )
    squares = jnp.sum(steered * steered, axis=1, keepdims=True)
    high, low = split_parts(squares, 2)
    slots = 2 * lanes + (-2 * lanes % 128)
    slot = jnp.arange(slots)[None, :]
    extra = jnp.where(slot == lane, high, jnp.where(slot == lane + lanes, low, 0.0))
    gained = jnp.concatenate([steered * attn_gain[None, :], extra], axis=1).astype(BF16)
    gained = gather_head(gained)
    local = residual.shape[1]
    partial = jnp.dot(gained[:, :local], w_query, preferred_element_type=F32)
    tail = gained[:, local:].astype(F32)

    columns = partial.shape[1] // 2
    mine = jnp.concatenate([take(partial, rep * columns, columns, 1), tail], axis=1)
    give = jnp.concatenate([take(partial, (1 - rep) * columns, columns, 1), tail], axis=1)
    total = mine + swap(give.astype(BF16), "rep", 1).astype(F32)
    send = total.astype(BF16)
    for bit in bits_of(seq_size):
        total, send = add_stage(total, swap(send, "seq", bit))
    squares = jnp.sum(total[:, columns:], axis=1)
    inverse = lax.rsqrt(squares / width + EPSILON)
    cosine, sine = rope_tables(prompt_length + suffix_lengths - 1, size)
    half_queries = total[:, :columns].reshape(rows, heads // 2, size) * inverse[:, None, None]
    half_queries = rotate(half_queries, cosine, sine).astype(BF16).reshape(rows, columns)
    queries = in_order(rep == 1, half_queries, swap(half_queries, "rep", 1), 1)
    queries = queries.reshape(rows, kv_local, heads_per_group, size)

    scale = 1.0 / math.sqrt(size)
    scores = (
        jnp.einsum("rkgd,pkd->rkgp", queries, prefix_keys, preferred_element_type=F32) * scale
    )
    highest = jnp.max(scores, axis=3)
    weights = jnp.exp(scores - highest[..., None])
    totals = jnp.sum(weights, axis=3)
    weighted = jnp.einsum(
        "rkgp,pkd->rkgd", weights.astype(BF16), prompt_value_rows, preferred_element_type=F32
    )
    prefix_out = (weighted / totals[..., None]).reshape(rows, heads, size)
    prefix_lse = (highest + jnp.log(totals)).reshape(rows, heads)
    own_queries = take(queries, first_own, share, 0)
    own_lengths = take(suffix_lengths, first_own, share, 0)
    live = (jnp.arange(suffix_tokens)[None, :] < own_lengths[:, None])[:, None, None, :]
    tail_scores = (
        jnp.einsum(
            "rkgd,rskd->rkgs", own_queries, private_suffix_keys, preferred_element_type=F32
        )
        * scale
    )
    tail_scores = jnp.where(live, tail_scores, -jnp.inf)
    tail_high = jnp.max(tail_scores, axis=3)
    tail_weights = jnp.where(live, jnp.exp(tail_scores - tail_high[..., None]), 0.0)
    tail_totals = jnp.sum(tail_weights, axis=3)
    tail_weighted = jnp.einsum(
        "rkgs,rskd->rkgd",
        tail_weights.astype(BF16),
        private_suffix_values,
        preferred_element_type=F32,
    )
    tail_out = (tail_weighted / tail_totals[..., None]).reshape(share, heads, size)
    tail_lse = (tail_high + jnp.log(tail_totals)).reshape(share, heads)
    own_out = take(prefix_out, first_own, share, 0)
    own_lse = take(prefix_lse, first_own, share, 0)
    own_out, own_lse = merge((own_out, own_lse), (tail_out, tail_lse))
    prefix_out = lax.dynamic_update_slice_in_dim(prefix_out, own_out, first_own, 0)
    prefix_lse = lax.dynamic_update_slice_in_dim(prefix_lse, own_lse, first_own, 0)

    half_heads = heads // 2
    state = (
        take(prefix_out, rep * half_heads, half_heads, 1),
        take(prefix_lse, rep * half_heads, half_heads, 1),
    )
    give = pack(
        take(prefix_out, (1 - rep) * half_heads, half_heads, 1),
        take(prefix_lse, (1 - rep) * half_heads, half_heads, 1),
    )
    out, lse = state
    lse = jnp.pad(lse, ((0, 0), (0, 128 - half_heads)))
    state = (out.reshape(rows, half_heads * size), lse)
    got = swap(give, "rep", 1)
    for bit in bits_of(seq_size):
        *state, send = merge_stage(state, got, half_heads, size, False)
        got = swap(send, "seq", bit)
    attended = merge_stage(state, got, half_heads, size, True)
    attended = in_order(rep == 1, attended, swap(attended, "rep", 1), 1)

    projected = jnp.dot(attended, w_output, preferred_element_type=F32)
    own_rows = take(projected, group * block_rows, block_rows, 0) + steered
    projected = lax.dynamic_update_slice_in_dim(projected, own_rows, group * block_rows, 0)
    middle = projected.astype(BF16)

    if groups == 2 and seq_size >= 2:
        half = seq_size // 2
        seq = lax.axis_index("seq")
        home = seq // half == group
        near, far = [], []
        for s in range(seq_size):
            g = s // half
            near.append((2 * s + 1 - g, 2 * s + g))
            near.append((2 * s + g, 2 * (s ^ half) + g))
            far.append((2 * s + 1 - g, 2 * (s ^ half) + g))
        got = lax.ppermute(middle, ("seq", "head"), near).astype(F32)
        away = lax.ppermute(middle, ("seq", "head"), far).astype(F32)
        middle = (got + jnp.where(home, middle.astype(F32), away)).astype(BF16)
        for bit in sorted(bits_of(half), reverse=True):
            middle = interleave((seq & bit) != 0, middle, swap(middle, "seq", bit), local)
        middle = interleave(rep == 1, middle, swap(middle, "rep", 1), local)
    else:
        for bit in bits_of(groups):
            middle = (middle.astype(F32) + swap(middle, "head", bit).astype(F32)).astype(BF16)
        middle = lax.all_gather(middle, LANES, axis=1, tiled=True)
        middle = take(middle, group * (width // groups), width // groups, 1)

    shard_width = width // groups
    middle_float = middle.astype(F32)
    gain = take(mlp_gain, group * shard_width, shard_width, 0)
    squares = jnp.sum(middle_float * middle_float, axis=1, keepdims=True)
    gained = (middle_float * gain[None, :]).astype(BF16)
    ff_local = w_gate.shape[1]
    gate = jnp.dot(gained, w_gate, preferred_element_type=F32)
    up = jnp.dot(gained, w_up, preferred_element_type=F32)
    total = jnp.concatenate([gate, up], axis=1)
    for bit in bits_of(groups):
        parts = jnp.concatenate(split_parts(squares, 3), axis=1)
        parts = jnp.pad(parts, ((0, 0), (0, 125)))
        got = swap(jnp.concatenate([total, parts], axis=1).astype(BF16), "head", bit).astype(F32)
        total = total + got[:, : 2 * ff_local]
        squares = squares + jnp.sum(got[:, 2 * ff_local :], axis=1, keepdims=True)
    total = total * lax.rsqrt(squares / width + EPSILON)
    hidden = jax.nn.silu(total[:, :ff_local]) * total[:, ff_local:]
    bits = lanes.bit_length() - 1
    hidden = hidden.reshape((2,) * bits + (share, ff_local))
    hidden = hidden.transpose(tuple(reversed(range(bits))) + (bits, bits + 1))
    hidden = hidden.reshape(rows, ff_local).astype(BF16)
    down = jnp.dot(hidden, w_down, preferred_element_type=F32)
    size_left = rows
    for axis, bit in [("rep", 1)] + [("seq", bit) for bit in bits_of(seq_size)]:
        size_left //= 2
        upper = (lax.axis_index(axis) & bit) != 0
        low, high = down[:size_left], down[size_left:]
        got = swap(jnp.where(upper, low, high).astype(BF16), axis, bit)
        down = jnp.where(upper, high, low) + got.astype(F32)
    own_middle = take(middle, first_own, share, 0).astype(F32)
    return (own_middle + down).astype(BF16)


def interleave(flag, mine, other, local):
    rows, wide = mine.shape
    mine = mine.reshape(rows, wide // local, 1, local)
    other = other.reshape(rows, wide // local, 1, local)
    return in_order(flag, mine, other, 2).reshape(rows, 2 * wide)


def solution(mesh):
    return jax.shard_map(
        shards,
        mesh=mesh,
        in_specs=(
            P(("parts", "head"), ("seq", "rep")),
            P(("parts", "head"), None),
            P(None, ("seq", "rep")),
            P(("seq", "rep")),
            P(),
            P(("seq", "rep"), "head"),
            P("head", ("seq", "rep")),
            P("head", ("seq", "rep")),
            P("head", ("seq", "rep")),
            P(("seq", "rep"), "head"),
            P(("parts", "seq", "rep"), "head", None),
            P(("parts", "seq", "rep"), "head", None),
            P(("parts", "seq", "rep"), None, "head", None),
            P(("parts", "seq", "rep"), None, "head", None),
            P("parts"),
        ),
        out_specs=P(("parts", "seq", "rep"), "head"),
        check_vma=False,
    )
```

```python
import functools
import math

import jax
import jax.numpy as jnp
from jax import lax
from jax.experimental import pallas as pl
from jax.experimental.pallas import tpu as pltpu
from jax.sharding import PartitionSpec as P

QUERY_HEADS = 64
KEY_VALUE_HEADS = 8
EPSILON = 1e-05
ROPE_BASE = 500000.0
LANES = ("seq", "rep")
ARRIVE_WORK, JOIN_WORK = 3_000_000_000, 1_000_000_000
F32 = jnp.float32
BF16 = jnp.bfloat16


def swap(x, axis, bit):
    size = lax.axis_size(axis)
    return lax.ppermute(x, axis, [(i, i ^ bit) for i in range(size)])


def bits_of(size):
    bit = 1
    while bit < size:
        yield bit
        bit *= 2


def take(x, start, size, axis):
    return lax.dynamic_slice_in_dim(x, start, size, axis)


def in_order(flag, mine, other, axis):
    first = jnp.where(flag, other, mine)
    second = jnp.where(flag, mine, other)
    return jnp.concatenate([first, second], axis=axis)


def split_parts(value, count):
    parts = []
    for _ in range(count):
        head = lax.reduce_precision(value, 8, 7)
        parts.append(head)
        value = value - head
    return parts


def local_call(body, outs, *args, specs=None, flops=3_000_000_000):
    return pl.pallas_call(
        body,
        out_shape=outs,
        in_specs=specs or [pl.BlockSpec(memory_space=pltpu.VMEM)] * len(args),
        cost_estimate=pl.CostEstimate(flops=flops, bytes_accessed=0, transcendentals=0),
        compiler_params=pltpu.CompilerParams(vmem_limit_bytes=4 << 20),
    )(*args)


def add_kernel(total_ref, *refs):
    *got_refs, next_ref, send_ref = refs
    total = total_ref[...]
    for got_ref in got_refs:
        total = total + got_ref[...].astype(F32)
    next_ref[...] = total
    send_ref[...] = total.astype(BF16)


def add_stage(total, gots):
    shapes = (
        jax.ShapeDtypeStruct(total.shape, F32),
        jax.ShapeDtypeStruct(total.shape, BF16),
    )
    return local_call(add_kernel, shapes, total, *gots)


def rope_kernel(width, total_ref, cosine_ref, sine_ref, *refs):
    *got_refs, out_ref = refs
    total = total_ref[...]
    for got_ref in got_refs:
        total = total + got_ref[...].astype(F32)
    wide = out_ref.shape[1]
    squares = jnp.sum(total[:, wide:], axis=1, keepdims=True)
    inverse = lax.rsqrt(squares / width + EPSILON)
    cosine, sine = cosine_ref[...], sine_ref[...]
    size = cosine.shape[1]
    for first in range(0, wide, size):
        head = total[:, first : first + size] * inverse
        turned = head * cosine + pltpu.roll(head, size // 2, 1) * sine
        out_ref[:, first : first + size] = turned.astype(BF16)


def arrive_kernel(half_lanes, flags_ref, mine_ref, near_ref, far_ref, out_ref):
    home = flags_ref[2] // half_lanes == flags_ref[1]
    other = jnp.where(home, mine_ref[...], far_ref[...])
    out_ref[...] = (near_ref[...].astype(F32) + other.astype(F32)).astype(BF16)


def arrive(half_lanes, flags, mine, near, far):
    smem = pl.BlockSpec(memory_space=pltpu.SMEM)
    vmem = pl.BlockSpec(memory_space=pltpu.VMEM)
    return local_call(
        functools.partial(arrive_kernel, half_lanes),
        jax.ShapeDtypeStruct(mine.shape, BF16),
        flags,
        mine,
        near,
        far,
        specs=[smem, vmem, vmem, vmem],
        flops=ARRIVE_WORK,
    )


def join_kernel(one_ref, two_ref, out_ref):
    cut = one_ref.shape[1]
    out_ref[:, :cut] = one_ref[...]
    out_ref[:, cut:] = two_ref[...]


def join(one, two):
    shape = (one.shape[0], one.shape[1] + two.shape[1])
    return local_call(join_kernel, jax.ShapeDtypeStruct(shape, BF16), one, two, flops=JOIN_WORK)


def parts_of(value, heads):
    lane = lax.broadcasted_iota(jnp.int32, value.shape, 1)
    value = jnp.where(lane < heads, value, 0.0)
    packed = jnp.zeros_like(value)
    for i in range(3):
        head = value.astype(BF16).astype(F32)
        packed = packed + (pltpu.roll(head, i * heads, 1) if i else head)
        value = value - head
    return packed


def joined(packed, heads):
    lanes = packed.shape[1]
    value = packed
    for i in range(1, 3):
        value = value + pltpu.roll(packed, lanes - i * heads, 1)
    return value


def merge_kernel(heads, size, last, out_ref, lse_ref, *refs):
    count = len(refs) - (1 if last else 3)
    got_refs, refs = refs[:count], refs[count:]
    wide = heads * size
    lses = [lse_ref[...]] + [joined(ref[:, wide:].astype(F32), heads) for ref in got_refs]
    high = functools.reduce(jnp.maximum, lses)
    weights = [jnp.exp(lse - high) for lse in lses]
    total = functools.reduce(jnp.add, weights)
    shares = [weight / total for weight in weights]
    for h in range(heads):
        cols = slice(h * size, (h + 1) * size)
        merged = shares[0][:, h : h + 1] * out_ref[:, cols]
        for share, ref in zip(shares[1:], got_refs):
            merged = merged + share[:, h : h + 1] * ref[:, cols].astype(F32)
        if last:
            refs[0][:, cols] = merged.astype(BF16)
        else:
            refs[0][:, cols] = merged
            refs[2][:, cols] = merged.astype(BF16)
    if not last:
        lse = high + jnp.log(total)
        refs[1][...] = lse
        refs[2][:, wide:] = parts_of(lse, heads).astype(BF16)


def merge_stage(state, gots, heads, size, last):
    out, lse = state
    rows = out.shape[0]
    wide = heads * size
    if last:
        outs = jax.ShapeDtypeStruct((rows, wide), BF16)
    else:
        outs = (
            jax.ShapeDtypeStruct((rows, wide), F32),
            jax.ShapeDtypeStruct(lse.shape, F32),
            jax.ShapeDtypeStruct((rows, wide + lse.shape[1]), BF16),
        )
    body = functools.partial(merge_kernel, heads, size, last)
    return local_call(body, outs, out, lse, *gots)


def rope_tables(positions, width):
    half = width // 2
    exponent = jnp.arange(half, dtype=F32) * (2.0 / width)
    frequency = jnp.exp(-math.log(ROPE_BASE) * exponent)
    angles = positions.astype(F32)[:, None] * frequency[None, :]
    cosine, sine = jnp.cos(angles), jnp.sin(angles)
    return jnp.concatenate([cosine, cosine], axis=1), jnp.concatenate([-sine, sine], axis=1)


def exchanges(size):
    bits = list(bits_of(size))
    if len(bits) < 2:
        return [[bit] for bit in bits]
    low, high = bits[-2:]
    return [[bit] for bit in bits[:-2]] + [[low, high, low | high]]


def merge(one, two):
    out_one, lse_one = one
    out_two, lse_two = two
    high = jnp.maximum(lse_one, lse_two)
    w_one = jnp.exp(lse_one - high)
    w_two = jnp.exp(lse_two - high)
    total = w_one + w_two
    out = out_one * (w_one / total)[..., None] + out_two * (w_two / total)[..., None]
    return out, high + jnp.log(total)


def pack(out, lse):
    rows, heads, size = out.shape
    parts = jnp.concatenate(split_parts(lse, 3), axis=1)
    pad = -parts.shape[1] % 128
    parts = jnp.pad(parts, ((0, 0), (0, pad)))
    return jnp.concatenate([out.reshape(rows, heads * size), parts], axis=1).astype(BF16)


def steps_of(size, most):
    step = min(size, most)
    while size % step or (step < size and step % 128):
        step -= 1
    return step


def weight_call(body, outs, weights, flags, *args):
    count = len(weights)
    total = sum(weight.size * weight.dtype.itemsize for weight in weights)

    def kernel(flags_ref, *refs):
        body(flags_ref, refs[:count], *refs[count:])

    return pl.pallas_call(
        kernel,
        out_shape=outs,
        in_specs=[pl.BlockSpec(memory_space=pltpu.SMEM)]
        + [pl.BlockSpec(memory_space=pltpu.VMEM)] * (count + len(args)),
        cost_estimate=pl.CostEstimate(flops=0, bytes_accessed=total, transcendentals=0),
        compiler_params=pltpu.CompilerParams(vmem_limit_bytes=total + (4 << 20)),
    )(flags, *weights, *args)


def seal_kernel(lanes, flags_ref, gained_ref, squares_ref, out_ref):
    local = gained_ref.shape[1]
    out_ref[:, :local] = gained_ref[...]
    squares = squares_ref[...]
    high = squares.astype(BF16).astype(F32)
    low = squares - high
    slot = lax.broadcasted_iota(jnp.int32, (squares.shape[0], out_ref.shape[1] - local), 1)
    lane = flags_ref[2]
    tail = jnp.where(slot == lane, high, jnp.where(slot == lane + lanes, low, 0.0))
    out_ref[:, local:] = tail.astype(BF16)


def query_kernel(local, flags_ref, weights, *refs):
    *x_refs, mine_ref, give_ref = refs
    (weight,) = weights
    x = x_refs[0][...]
    if len(x_refs) == 2:
        other = x_refs[1][...]
        second = flags_ref[1] == 1
        x = jnp.concatenate([jnp.where(second, other, x), jnp.where(second, x, other)], axis=0)
    half = weight.shape[1] // 2
    upper = flags_ref[0] == 1
    step = steps_of(half, 1024)
    for c in range(0, half, step):
        low = jnp.dot(x[:, :local], weight[:, c : c + step], preferred_element_type=F32)
        high = jnp.dot(
            x[:, :local], weight[:, half + c : half + c + step], preferred_element_type=F32
        )
        mine_ref[:, c : c + step] = jnp.where(upper, high, low)
        give_ref[:, c : c + step] = jnp.where(upper, low, high).astype(BF16)
    mine_ref[:, half:] = x[:, local:].astype(F32)
    give_ref[:, half:] = x[:, local:]


def output_kernel(flags_ref, weights, mine_ref, other_ref, steered_ref, out_ref):
    (weight,) = weights
    half = weight.shape[0] // 2
    step = steps_of(half, 1024)
    total = jnp.zeros(out_ref.shape, F32)
    upper = flags_ref[0] == 1
    for k in range(0, half, step):
        cols = slice(k, k + step)
        mine, other = mine_ref[:, cols], other_ref[:, cols]
        low, high = jnp.where(upper, other, mine), jnp.where(upper, mine, other)
        total += jnp.dot(low, weight[k : k + step, :], preferred_element_type=F32)
        total += jnp.dot(high, weight[half + k : half + k + step, :], preferred_element_type=F32)
    block = steered_ref.shape[0]
    for g in range(out_ref.shape[0] // block):
        rows = slice(g * block, (g + 1) * block)
        own = jnp.where(flags_ref[1] == g, steered_ref[...], 0.0)
        out_ref[rows, :] = (total[rows] + own).astype(BF16)


def wide_kernel(local, places, flags_ref, weights, x_ref, gain_ref, *outs):
    gate, up, tail_ref, own_ref = outs
    wide = x_ref.shape[1]
    x = x_ref[...].astype(F32)
    squares = jnp.sum(x * x, axis=1, keepdims=True)
    lane = lax.broadcasted_iota(jnp.int32, tail_ref.shape, 1)
    tail_ref[...] = jnp.where(lane == 0, squares, 0.0)
    sums = [None] * len(weights)
    row = lax.broadcasted_iota(jnp.int32, (x.shape[0], local), 0)
    for b in range(wide // local):
        place = places(flags_ref, b)
        start = pl.multiple_of(place * local, local)
        whole = flags_ref[1] * weights[0].shape[0] + place * local
        scale = gain_ref[:, pl.ds(pl.multiple_of(whole, local), local)]
        block = x[:, b * local : (b + 1) * local]
        part = (block * scale).astype(BF16)
        for i in range(own_ref.shape[0]):
            own = jnp.where(row == flags_ref[2] * own_ref.shape[0] + i, block, 0.0)
            own_ref[i : i + 1, pl.ds(start, local)] = jnp.sum(own, axis=0, keepdims=True)
        for n, weight in enumerate(weights):
            got = jnp.dot(part, weight[pl.ds(start, local), :], preferred_element_type=F32)
            sums[n] = got if sums[n] is None else sums[n] + got
    gate[...] = sums[0]
    up[...] = sums[1]


def wide_call(weights, places, local, share, flags, x, gain):
    rows = x.shape[0]
    outs = [jax.ShapeDtypeStruct((rows, weights[0].shape[1]), F32)] * 2
    outs.append(jax.ShapeDtypeStruct((rows, 128), F32))
    outs.append(jax.ShapeDtypeStruct((share, x.shape[1]), F32))
    body = functools.partial(wide_kernel, local, places)
    return weight_call(body, tuple(outs), weights, flags, x, gain)


def pack_kernel(gate_ref, up_ref, tail_ref, out_ref):
    cut = gate_ref.shape[1]
    out_ref[:, :cut] = gate_ref[...].astype(BF16)
    out_ref[:, cut : 2 * cut] = up_ref[...].astype(BF16)
    out_ref[:, 2 * cut :] = parts_of(tail_ref[...], 1).astype(BF16)


def combine_kernel(gate_ref, up_ref, tail_ref, got_ref, gate_out, up_out, tail_out):
    cut = gate_ref.shape[1]
    gate_out[...] = gate_ref[...] + got_ref[:, :cut].astype(F32)
    up_out[...] = up_ref[...] + got_ref[:, cut : 2 * cut].astype(F32)
    tail_out[...] = tail_ref[...] + joined(got_ref[:, 2 * cut :].astype(F32), 1)


def down_kernel(lanes, width, flags_ref, weights, gate_ref, up_ref, tail_ref, mine_ref, give_ref):
    (weight,) = weights
    rows, depth = gate_ref.shape
    inverse = lax.rsqrt(tail_ref[:, :1] / width + EPSILON)
    gate = gate_ref[...] * inverse
    up = up_ref[...] * inverse
    hidden = (gate / (1.0 + jnp.exp(-gate)) * up).astype(BF16)
    share = rows // lanes
    row = lax.broadcasted_iota(jnp.int32, (rows, rows), 0)
    source = lax.broadcasted_iota(jnp.int32, (rows, rows), 1)
    left, turned = row // share, jnp.zeros_like(row)
    for _ in range(lanes.bit_length() - 1):
        turned = turned * 2 + left % 2
        left = left // 2
    turned = turned * share + row % share
    order = (turned == source).astype(F32).astype(BF16)
    hidden = jnp.dot(order, hidden, preferred_element_type=F32).astype(BF16)
    half = rows // 2
    upper = flags_ref[0] == 1
    step = steps_of(weight.shape[1], 1024)
    for c in range(0, weight.shape[1], step):
        cols = slice(c, c + step)
        block = jnp.dot(hidden, weight[:, cols], preferred_element_type=F32)
        low, high = block[:half], block[half:]
        mine_ref[:, cols] = jnp.where(upper, high, low)
        give_ref[:, cols] = jnp.where(upper, low, high).astype(BF16)


def shards(
    residual,
    coefficients,
    directions,
    attn_gain,
    mlp_gain,
    w_query,
    w_output,
    w_gate,
    w_up,
    w_down,
    prefix_keys,
    prompt_value_rows,
    private_suffix_keys,
    private_suffix_values,
    suffix_lengths,
):
    lanes = lax.axis_size(LANES)
    lane = lax.axis_index(LANES)
    rep = lax.axis_index("rep")
    seq_size = lax.axis_size("seq")
    groups = lax.axis_size("head")
    group = lax.axis_index("head")
    block_rows = residual.shape[0]
    rows = block_rows * groups
    share = rows // lanes
    first_own = lane * share
    width = w_gate.shape[0] * groups
    prompt_length = prefix_keys.shape[0] * lanes
    kv_local, size = prefix_keys.shape[1:]
    heads_per_group = QUERY_HEADS // KEY_VALUE_HEADS
    heads = kv_local * heads_per_group
    suffix_tokens = private_suffix_keys.shape[1]

    local = residual.shape[1]
    slots = 2 * lanes + (-2 * lanes % 128)
    flags = jnp.stack([rep, group, lane]).astype(jnp.int32)
    smem = pl.BlockSpec(memory_space=pltpu.SMEM)
    vmem = pl.BlockSpec(memory_space=pltpu.VMEM)
    steered = residual.astype(F32) + jnp.dot(
        coefficients, directions, precision=lax.Precision.HIGHEST
    )
    squares = jnp.sum(steered * steered, axis=1, keepdims=True)
    gained = local_call(
        functools.partial(seal_kernel, lanes),
        jax.ShapeDtypeStruct((block_rows, local + slots), BF16),
        flags,
        (steered * attn_gain[None, :]).astype(BF16),
        squares,
        specs=[smem, vmem, vmem],
    )
    if groups == 2:
        gained = (gained, swap(gained, "head", 1))
    else:
        gained = (lax.all_gather(gained, "head", axis=0, tiled=True),)

    columns = w_query.shape[1] // 2
    wide = columns + slots
    mine, give = weight_call(
        functools.partial(query_kernel, local),
        (jax.ShapeDtypeStruct((rows, wide), F32), jax.ShapeDtypeStruct((rows, wide), BF16)),
        (w_query,),
        flags,
        *gained,
    )
    total = mine + swap(give, "rep", 1).astype(F32)
    send = total.astype(BF16)
    cosine, sine = rope_tables(prompt_length + suffix_lengths - 1, size)
    plan = exchanges(seq_size)
    for bits in plan[:-1]:
        total, send = add_stage(total, [swap(send, "seq", bit) for bit in bits])
    half_queries = local_call(
        functools.partial(rope_kernel, width),
        jax.ShapeDtypeStruct((rows, columns), BF16),
        total,
        cosine,
        sine,
        *[swap(send, "seq", bit) for bit in plan[-1]],
    )
    queries = in_order(rep == 1, half_queries, swap(half_queries, "rep", 1), 1)
    queries = queries.reshape(rows, kv_local, heads_per_group, size)

    scale = 1.0 / math.sqrt(size)
    scores = (
        jnp.einsum("rkgd,pkd->rkgp", queries, prefix_keys, preferred_element_type=F32) * scale
    )
    highest = jnp.max(scores, axis=3)
    weights = jnp.exp(scores - highest[..., None])
    totals = jnp.sum(weights, axis=3)
    weighted = jnp.einsum(
        "rkgp,pkd->rkgd", weights.astype(BF16), prompt_value_rows, preferred_element_type=F32
    )
    prefix_out = (weighted / totals[..., None]).reshape(rows, heads, size)
    prefix_lse = (highest + jnp.log(totals)).reshape(rows, heads)
    own_queries = take(queries, first_own, share, 0)
    own_lengths = take(suffix_lengths, first_own, share, 0)
    live = (jnp.arange(suffix_tokens)[None, :] < own_lengths[:, None])[:, None, None, :]
    tail_scores = (
        jnp.einsum(
            "rkgd,rskd->rkgs", own_queries, private_suffix_keys, preferred_element_type=F32
        )
        * scale
    )
    tail_scores = jnp.where(live, tail_scores, -jnp.inf)
    tail_high = jnp.max(tail_scores, axis=3)
    tail_weights = jnp.where(live, jnp.exp(tail_scores - tail_high[..., None]), 0.0)
    tail_totals = jnp.sum(tail_weights, axis=3)
    tail_weighted = jnp.einsum(
        "rkgs,rskd->rkgd",
        tail_weights.astype(BF16),
        private_suffix_values,
        preferred_element_type=F32,
    )
    tail_out = (tail_weighted / tail_totals[..., None]).reshape(share, heads, size)
    tail_lse = (tail_high + jnp.log(tail_totals)).reshape(share, heads)
    own_out = take(prefix_out, first_own, share, 0)
    own_lse = take(prefix_lse, first_own, share, 0)
    own_out, own_lse = merge((own_out, own_lse), (tail_out, tail_lse))
    prefix_out = lax.dynamic_update_slice_in_dim(prefix_out, own_out, first_own, 0)
    prefix_lse = lax.dynamic_update_slice_in_dim(prefix_lse, own_lse, first_own, 0)

    half_heads = heads // 2
    state = (
        take(prefix_out, rep * half_heads, half_heads, 1),
        take(prefix_lse, rep * half_heads, half_heads, 1),
    )
    give = pack(
        take(prefix_out, (1 - rep) * half_heads, half_heads, 1),
        take(prefix_lse, (1 - rep) * half_heads, half_heads, 1),
    )
    out, lse = state
    lse = jnp.pad(lse, ((0, 0), (0, 128 - half_heads)))
    state = (out.reshape(rows, half_heads * size), lse)
    gots = [swap(give, "rep", 1)]
    for bits in plan:
        *state, send = merge_stage(state, gots, half_heads, size, False)
        gots = [swap(send, "seq", bit) for bit in bits]
    attended = merge_stage(state, gots, half_heads, size, True)

    other = swap(attended, "rep", 1)
    middle = weight_call(
        output_kernel,
        jax.ShapeDtypeStruct((rows, local), BF16),
        (w_output,),
        flags,
        attended,
        other,
        steered,
    )

    shard_width = width // groups
    weights = (w_gate, w_up)
    gain = mlp_gain[None, :]
    if groups == 2 and seq_size >= 2:
        half = seq_size // 2
        near, far = [], []
        for s in range(seq_size):
            g = s // half
            near.append((2 * s + 1 - g, 2 * s + g))
            near.append((2 * s + g, 2 * (s ^ half) + g))
            far.append((2 * s + 1 - g, 2 * (s ^ half) + g))
        got = lax.ppermute(middle, ("seq", "head"), near)
        away = lax.ppermute(middle, ("seq", "head"), far)
        middle = arrive(lanes // 2, flags, middle, got, away)
        stages = [("seq", bit) for bit in sorted(bits_of(half), reverse=True)] + [("rep", 1)]
        turns = [0]
        for axis, bit in stages:
            middle = join(middle, swap(middle, axis, bit))
            turns += [turn ^ (1 if axis == "rep" else 2 * bit) for turn in turns]

        def places(flags_ref, b):
            return (flags_ref[2] % (lanes // 2)) ^ turns[b]

    else:
        for bit in bits_of(groups):
            middle = (middle.astype(F32) + swap(middle, "head", bit).astype(F32)).astype(BF16)
        middle = lax.all_gather(middle, LANES, axis=1, tiled=True)
        middle = take(middle, group * shard_width, shard_width, 1)

        def places(flags_ref, b):
            return b

    gate, up, tail, own_middle = wide_call(weights, places, local, share, flags, middle, gain)

    ff_local = w_gate.shape[1]
    for bit in bits_of(groups):
        send = local_call(
            pack_kernel, jax.ShapeDtypeStruct((rows, 2 * ff_local + 128), BF16), gate, up, tail
        )
        got = swap(send, "head", bit)
        shapes = tuple(jax.ShapeDtypeStruct(x.shape, F32) for x in (gate, up, tail))
        gate, up, tail = local_call(combine_kernel, shapes, gate, up, tail, got)
    half_rows = rows // 2
    down, give = weight_call(
        functools.partial(down_kernel, lanes, width),
        (
            jax.ShapeDtypeStruct((half_rows, shard_width), F32),
            jax.ShapeDtypeStruct((half_rows, shard_width), BF16),
        ),
        (w_down,),
        flags,
        gate,
        up,
        tail,
    )
    down = down + swap(give, "rep", 1).astype(F32)
    size_left = half_rows
    bits = list(bits_of(seq_size))
    seq = lax.axis_index("seq")
    for bit in bits[:-2]:
        size_left //= 2
        upper = (seq & bit) != 0
        low, high = down[:size_left], down[size_left:]
        got = swap(jnp.where(upper, low, high).astype(BF16), "seq", bit)
        down = jnp.where(upper, high, low) + got.astype(F32)
    unit = bits[-2]
    quarters = down.reshape(2, 2, share, shard_width)

    def quarter(place):
        one, two = place // unit % 2, place // (2 * unit) % 2
        part = lax.dynamic_index_in_dim(quarters, one, 0, keepdims=False)
        return lax.dynamic_index_in_dim(part, two, 0, keepdims=False)

    down = quarter(seq)
    gots = [
        swap(quarter(seq ^ bit).astype(BF16), "seq", bit)
        for bit in (unit, 2 * unit, 3 * unit)
    ]
    for got in gots:
        down = down + got.astype(F32)
    return (own_middle + down).astype(BF16)


def solution(mesh):
    return jax.shard_map(
        shards,
        mesh=mesh,
        in_specs=(
            P(("parts", "head"), ("seq", "rep")),
            P(("parts", "head"), None),
            P(None, ("seq", "rep")),
            P(("seq", "rep")),
            P(),
            P(("seq", "rep"), "head"),
            P("head", ("seq", "rep")),
            P("head", ("seq", "rep")),
            P("head", ("seq", "rep")),
            P(("seq", "rep"), "head"),
            P(("parts", "seq", "rep"), "head", None),
            P(("parts", "seq", "rep"), "head", None),
            P(("parts", "seq", "rep"), None, "head", None),
            P(("parts", "seq", "rep"), None, "head", None),
            P("parts"),
        ),
        out_specs=P(("parts", "seq", "rep"), "head"),
        check_vma=False,
    )
```

```python
import functools
import math

import jax
import jax.numpy as jnp
from jax import lax
from jax.experimental import pallas as pl
from jax.experimental.pallas import tpu as pltpu
from jax.sharding import PartitionSpec as P


QUERY_HEADS = 64
KEY_VALUE_HEADS = 8
EPSILON = 1e-05
ROPE_BASE = 500000.0
LANES = ("seq", "rep")
ARRIVE_WORK, JOIN_WORK = 3_000_000_000, 1_000_000_000
F32 = jnp.float32
BF16 = jnp.bfloat16


def swap(x, axis, bit):
    size = lax.axis_size(axis)
    return lax.ppermute(x, axis, [(i, i ^ bit) for i in range(size)])


def bits_of(size):
    bit = 1
    while bit < size:
        yield bit
        bit *= 2


def lane_index():
    return lax.axis_index("seq") * lax.axis_size("rep") + lax.axis_index("rep")


def take(x, start, size, axis):
    return lax.dynamic_slice_in_dim(x, start, size, axis)


def in_order(flag, mine, other, axis):
    first = jnp.where(flag, other, mine)
    second = jnp.where(flag, mine, other)
    return jnp.concatenate([first, second], axis=axis)


def split_parts(value, count):
    parts = []
    for _ in range(count):
        head = lax.reduce_precision(value, 8, 7)
        parts.append(head)
        value = value - head
    return parts


def local_call(body, outs, *args, flops=3_000_000_000):
    return pl.pallas_call(
        body,
        out_shape=outs,
        in_specs=[pl.BlockSpec(memory_space=pltpu.VMEM)] * len(args),
        cost_estimate=pl.CostEstimate(flops=flops, bytes_accessed=0, transcendentals=0),
        compiler_params=pltpu.CompilerParams(vmem_limit_bytes=4 << 20),
    )(*args)


def add_kernel(total_ref, *refs):
    *got_refs, next_ref, send_ref = refs
    total = total_ref[...]
    for got_ref in got_refs:
        total = total + got_ref[...].astype(F32)
    next_ref[...] = total
    send_ref[...] = total.astype(BF16)


def add_stage(total, gots):
    shapes = (
        jax.ShapeDtypeStruct(total.shape, F32),
        jax.ShapeDtypeStruct(total.shape, BF16),
    )
    return local_call(add_kernel, shapes, total, *gots)


def rope_kernel(width, total_ref, cosine_ref, sine_ref, *refs):
    *got_refs, out_ref = refs
    total = total_ref[...]
    for got_ref in got_refs:
        total = total + got_ref[...].astype(F32)
    wide = out_ref.shape[1]
    squares = jnp.sum(total[:, wide:], axis=1, keepdims=True)
    inverse = lax.rsqrt(squares / width + EPSILON)
    cosine, sine = cosine_ref[...], sine_ref[...]
    size = cosine.shape[1]
    for first in range(0, wide, size):
        head = total[:, first : first + size] * inverse
        turned = head * cosine + pltpu.roll(head, size // 2, 1) * sine
        out_ref[:, first : first + size] = turned.astype(BF16)


def arrive_kernel(half_lanes, mine_ref, near_ref, far_ref, out_ref):
    home = lane_index() // half_lanes == lax.axis_index("head")
    other = jnp.where(home, mine_ref[...], far_ref[...])
    out_ref[...] = (near_ref[...].astype(F32) + other.astype(F32)).astype(BF16)


def arrive(half_lanes, mine, near, far):
    return local_call(
        functools.partial(arrive_kernel, half_lanes),
        jax.ShapeDtypeStruct(mine.shape, BF16),
        mine,
        near,
        far,
        flops=ARRIVE_WORK,
    )


def join_kernel(one_ref, two_ref, out_ref):
    cut = one_ref.shape[1]
    out_ref[:, :cut] = one_ref[...]
    out_ref[:, cut:] = two_ref[...]


def join(one, two):
    shape = (one.shape[0], one.shape[1] + two.shape[1])
    return local_call(join_kernel, jax.ShapeDtypeStruct(shape, BF16), one, two, flops=JOIN_WORK)


def parts_of(value, heads):
    lane = lax.broadcasted_iota(jnp.int32, value.shape, 1)
    value = jnp.where(lane < heads, value, 0.0)
    packed = jnp.zeros_like(value)
    for i in range(3):
        head = value.astype(BF16).astype(F32)
        packed = packed + (pltpu.roll(head, i * heads, 1) if i else head)
        value = value - head
    return packed


def joined(packed, heads):
    lanes = packed.shape[1]
    value = packed
    for i in range(1, 3):
        value = value + pltpu.roll(packed, lanes - i * heads, 1)
    return value


def merge_kernel(heads, size, last, out_ref, lse_ref, *refs):
    count = len(refs) - (1 if last else 3)
    got_refs, refs = refs[:count], refs[count:]
    wide = heads * size
    lses = [lse_ref[...]] + [joined(ref[:, wide:].astype(F32), heads) for ref in got_refs]
    high = functools.reduce(jnp.maximum, lses)
    weights = [jnp.exp(lse - high) for lse in lses]
    total = functools.reduce(jnp.add, weights)
    shares = [weight / total for weight in weights]
    for h in range(heads):
        cols = slice(h * size, (h + 1) * size)
        merged = shares[0][:, h : h + 1] * out_ref[:, cols]
        for share, ref in zip(shares[1:], got_refs):
            merged = merged + share[:, h : h + 1] * ref[:, cols].astype(F32)
        if last:
            refs[0][:, cols] = merged.astype(BF16)
        else:
            refs[0][:, cols] = merged
            refs[2][:, cols] = merged.astype(BF16)
    if not last:
        lse = high + jnp.log(total)
        refs[1][...] = lse
        refs[2][:, wide:] = parts_of(lse, heads).astype(BF16)


def merge_stage(state, gots, heads, size, last):
    out, lse = state
    rows = out.shape[0]
    wide = heads * size
    if last:
        outs = jax.ShapeDtypeStruct((rows, wide), BF16)
    else:
        outs = (
            jax.ShapeDtypeStruct((rows, wide), F32),
            jax.ShapeDtypeStruct(lse.shape, F32),
            jax.ShapeDtypeStruct((rows, wide + lse.shape[1]), BF16),
        )
    body = functools.partial(merge_kernel, heads, size, last)
    return local_call(body, outs, out, lse, *gots)


def rope_tables(positions, width):
    half = width // 2
    exponent = jnp.arange(half, dtype=F32) * (2.0 / width)
    frequency = jnp.exp(-math.log(ROPE_BASE) * exponent)
    angles = positions.astype(F32)[:, None] * frequency[None, :]
    cosine, sine = jnp.cos(angles), jnp.sin(angles)
    return jnp.concatenate([cosine, cosine], axis=1), jnp.concatenate([-sine, sine], axis=1)


def exchanges(size):
    bits = list(bits_of(size))
    if len(bits) < 2:
        return [[bit] for bit in bits]
    low, high = bits[-2:]
    return [[bit] for bit in bits[:-2]] + [[low, high, low | high]]


def merge(one, two):
    out_one, lse_one = one
    out_two, lse_two = two
    high = jnp.maximum(lse_one, lse_two)
    w_one = jnp.exp(lse_one - high)
    w_two = jnp.exp(lse_two - high)
    total = w_one + w_two
    out = out_one * (w_one / total)[..., None] + out_two * (w_two / total)[..., None]
    return out, high + jnp.log(total)


def pack(out, lse):
    rows, heads, size = out.shape
    parts = jnp.concatenate(split_parts(lse, 3), axis=1)
    pad = -parts.shape[1] % 128
    parts = jnp.pad(parts, ((0, 0), (0, pad)))
    return jnp.concatenate([out.reshape(rows, heads * size), parts], axis=1).astype(BF16)


def steps_of(size, most):
    step = min(size, most)
    while size % step or (step < size and step % 128):
        step -= 1
    return step


def weight_call(body, outs, weights, *args):
    count = len(weights)
    total = sum(weight.size * weight.dtype.itemsize for weight in weights)

    def kernel(*refs):
        body(refs[:count], *refs[count:])

    return pl.pallas_call(
        kernel,
        out_shape=outs,
        in_specs=[pl.BlockSpec(memory_space=pltpu.VMEM)] * (count + len(args)),
        cost_estimate=pl.CostEstimate(flops=0, bytes_accessed=total, transcendentals=0),
        compiler_params=pltpu.CompilerParams(vmem_limit_bytes=total + (4 << 20)),
    )(*weights, *args)


def seal_kernel(lanes, gained_ref, squares_ref, out_ref):
    local = gained_ref.shape[1]
    out_ref[:, :local] = gained_ref[...]
    squares = squares_ref[...]
    high = squares.astype(BF16).astype(F32)
    low = squares - high
    slot = lax.broadcasted_iota(jnp.int32, (squares.shape[0], out_ref.shape[1] - local), 1)
    lane = lane_index()
    tail = jnp.where(slot == lane, high, jnp.where(slot == lane + lanes, low, 0.0))
    out_ref[:, local:] = tail.astype(BF16)


def query_kernel(local, weights, *refs):
    *x_refs, mine_ref, give_ref = refs
    (weight,) = weights
    x = x_refs[0][...]
    if len(x_refs) == 2:
        other = x_refs[1][...]
        second = lax.axis_index("head") == 1
        x = jnp.concatenate([jnp.where(second, other, x), jnp.where(second, x, other)], axis=0)
    half = weight.shape[1] // 2
    upper = lax.axis_index("rep") == 1
    step = steps_of(half, 1024)
    for c in range(0, half, step):
        low = jnp.dot(x[:, :local], weight[:, c : c + step], preferred_element_type=F32)
        high = jnp.dot(
            x[:, :local], weight[:, half + c : half + c + step], preferred_element_type=F32
        )
        mine_ref[:, c : c + step] = jnp.where(upper, high, low)
        give_ref[:, c : c + step] = jnp.where(upper, low, high).astype(BF16)
    mine_ref[:, half:] = x[:, local:].astype(F32)
    give_ref[:, half:] = x[:, local:]


def output_kernel(weights, mine_ref, other_ref, steered_ref, out_ref):
    (weight,) = weights
    half = weight.shape[0] // 2
    step = steps_of(half, 1024)
    total = jnp.zeros(out_ref.shape, F32)
    upper = lax.axis_index("rep") == 1
    for k in range(0, half, step):
        cols = slice(k, k + step)
        mine, other = mine_ref[:, cols], other_ref[:, cols]
        low, high = jnp.where(upper, other, mine), jnp.where(upper, mine, other)
        total += jnp.dot(low, weight[k : k + step, :], preferred_element_type=F32)
        total += jnp.dot(high, weight[half + k : half + k + step, :], preferred_element_type=F32)
    block = steered_ref.shape[0]
    for g in range(out_ref.shape[0] // block):
        rows = slice(g * block, (g + 1) * block)
        own = jnp.where(lax.axis_index("head") == g, steered_ref[...], 0.0)
        out_ref[rows, :] = (total[rows] + own).astype(BF16)


def wide_kernel(local, places, weights, x_ref, gain_ref, *outs):
    gate, up, tail_ref, own_ref = outs
    wide = x_ref.shape[1]
    x = x_ref[...].astype(F32)
    squares = jnp.sum(x * x, axis=1, keepdims=True)
    lane = lax.broadcasted_iota(jnp.int32, tail_ref.shape, 1)
    tail_ref[...] = jnp.where(lane == 0, squares, 0.0)
    sums = [None] * len(weights)
    row = lax.broadcasted_iota(jnp.int32, (x.shape[0], local), 0)
    for b in range(wide // local):
        place = places(b)
        start = pl.multiple_of(place * local, local)
        whole = lax.axis_index("head") * weights[0].shape[0] + place * local
        scale = gain_ref[:, pl.ds(pl.multiple_of(whole, local), local)]
        block = x[:, b * local : (b + 1) * local]
        part = (block * scale).astype(BF16)
        for i in range(own_ref.shape[0]):
            own = jnp.where(row == lane_index() * own_ref.shape[0] + i, block, 0.0)
            own_ref[i : i + 1, pl.ds(start, local)] = jnp.sum(own, axis=0, keepdims=True)
        for n, weight in enumerate(weights):
            got = jnp.dot(part, weight[pl.ds(start, local), :], preferred_element_type=F32)
            sums[n] = got if sums[n] is None else sums[n] + got
    gate[...] = sums[0]
    up[...] = sums[1]


def wide_call(weights, places, local, share, x, gain):
    rows = x.shape[0]
    outs = [jax.ShapeDtypeStruct((rows, weights[0].shape[1]), F32)] * 2
    outs.append(jax.ShapeDtypeStruct((rows, 128), F32))
    outs.append(jax.ShapeDtypeStruct((share, x.shape[1]), F32))
    body = functools.partial(wide_kernel, local, places)
    return weight_call(body, tuple(outs), weights, x, gain)


def pack_kernel(gate_ref, up_ref, tail_ref, out_ref):
    cut = gate_ref.shape[1]
    out_ref[:, :cut] = gate_ref[...].astype(BF16)
    out_ref[:, cut : 2 * cut] = up_ref[...].astype(BF16)
    out_ref[:, 2 * cut :] = parts_of(tail_ref[...], 1).astype(BF16)


def combine_kernel(gate_ref, up_ref, tail_ref, got_ref, gate_out, up_out, tail_out):
    cut = gate_ref.shape[1]
    gate_out[...] = gate_ref[...] + got_ref[:, :cut].astype(F32)
    up_out[...] = up_ref[...] + got_ref[:, cut : 2 * cut].astype(F32)
    tail_out[...] = tail_ref[...] + joined(got_ref[:, 2 * cut :].astype(F32), 1)


def down_kernel(lanes, width, weights, gate_ref, up_ref, tail_ref, mine_ref, give_ref):
    (weight,) = weights
    rows, _ = gate_ref.shape
    inverse = lax.rsqrt(tail_ref[:, :1] / width + EPSILON)
    gate = gate_ref[...] * inverse
    up = up_ref[...] * inverse
    hidden = (gate / (1.0 + jnp.exp(-gate)) * up).astype(BF16)
    share = rows // lanes
    row = lax.broadcasted_iota(jnp.int32, (rows, rows), 0)
    source = lax.broadcasted_iota(jnp.int32, (rows, rows), 1)
    left, turned = row // share, jnp.zeros_like(row)
    for _ in range(lanes.bit_length() - 1):
        turned = turned * 2 + left % 2
        left = left // 2
    turned = turned * share + row % share
    order = (turned == source).astype(F32).astype(BF16)
    hidden = jnp.dot(order, hidden, preferred_element_type=F32).astype(BF16)
    half = rows // 2
    upper = lax.axis_index("rep") == 1
    step = steps_of(weight.shape[1], 1024)
    for c in range(0, weight.shape[1], step):
        cols = slice(c, c + step)
        block = jnp.dot(hidden, weight[:, cols], preferred_element_type=F32)
        low, high = block[:half], block[half:]
        mine_ref[:, cols] = jnp.where(upper, high, low)
        give_ref[:, cols] = jnp.where(upper, low, high).astype(BF16)


def shards(
    residual,
    coefficients,
    directions,
    attn_gain,
    mlp_gain,
    w_query,
    w_output,
    w_gate,
    w_up,
    w_down,
    prefix_keys,
    prompt_value_rows,
    private_suffix_keys,
    private_suffix_values,
    suffix_lengths,
):
    lanes = lax.axis_size(LANES)
    lane = lax.axis_index(LANES)
    rep = lax.axis_index("rep")
    seq_size = lax.axis_size("seq")
    groups = lax.axis_size("head")
    group = lax.axis_index("head")
    block_rows = residual.shape[0]
    rows = block_rows * groups
    share = rows // lanes
    first_own = lane * share
    width = w_gate.shape[0] * groups
    prompt_length = prefix_keys.shape[0] * lanes
    kv_local, size = prefix_keys.shape[1:]
    heads_per_group = QUERY_HEADS // KEY_VALUE_HEADS
    heads = kv_local * heads_per_group
    suffix_tokens = private_suffix_keys.shape[1]

    local = residual.shape[1]
    slots = 2 * lanes + (-2 * lanes % 128)
    steered = residual.astype(F32) + jnp.dot(
        coefficients, directions, precision=lax.Precision.HIGHEST
    )
    squares = jnp.sum(steered * steered, axis=1, keepdims=True)
    gained = local_call(
        functools.partial(seal_kernel, lanes),
        jax.ShapeDtypeStruct((block_rows, local + slots), BF16),
        (steered * attn_gain[None, :]).astype(BF16),
        squares,
    )
    if groups == 2:
        gained = (gained, swap(gained, "head", 1))
    else:
        gained = (lax.all_gather(gained, "head", axis=0, tiled=True),)

    columns = w_query.shape[1] // 2
    wide = columns + slots
    mine, give = weight_call(
        functools.partial(query_kernel, local),
        (jax.ShapeDtypeStruct((rows, wide), F32), jax.ShapeDtypeStruct((rows, wide), BF16)),
        (w_query,),
        *gained,
    )
    total = mine + swap(give, "rep", 1).astype(F32)
    send = total.astype(BF16)
    cosine, sine = rope_tables(prompt_length + suffix_lengths - 1, size)
    plan = exchanges(seq_size)
    for bits in plan[:-1]:
        total, send = add_stage(total, [swap(send, "seq", bit) for bit in bits])
    half_queries = local_call(
        functools.partial(rope_kernel, width),
        jax.ShapeDtypeStruct((rows, columns), BF16),
        total,
        cosine,
        sine,
        *[swap(send, "seq", bit) for bit in plan[-1]],
    )
    queries = in_order(rep == 1, half_queries, swap(half_queries, "rep", 1), 1)
    queries = queries.reshape(rows, kv_local, heads_per_group, size)

    scale = 1.0 / math.sqrt(size)
    scores = (
        jnp.einsum("rkgd,pkd->rkgp", queries, prefix_keys, preferred_element_type=F32) * scale
    )
    highest = jnp.max(scores, axis=3)
    weights = jnp.exp(scores - highest[..., None])
    totals = jnp.sum(weights, axis=3)
    weighted = jnp.einsum(
        "rkgp,pkd->rkgd", weights.astype(BF16), prompt_value_rows, preferred_element_type=F32
    )
    prefix_out = (weighted / totals[..., None]).reshape(rows, heads, size)
    prefix_lse = (highest + jnp.log(totals)).reshape(rows, heads)
    own_queries = take(queries, first_own, share, 0)
    own_lengths = take(suffix_lengths, first_own, share, 0)
    live = (jnp.arange(suffix_tokens)[None, :] < own_lengths[:, None])[:, None, None, :]
    tail_scores = (
        jnp.einsum(
            "rkgd,rskd->rkgs", own_queries, private_suffix_keys, preferred_element_type=F32
        )
        * scale
    )
    tail_scores = jnp.where(live, tail_scores, -jnp.inf)
    tail_high = jnp.max(tail_scores, axis=3)
    tail_weights = jnp.where(live, jnp.exp(tail_scores - tail_high[..., None]), 0.0)
    tail_totals = jnp.sum(tail_weights, axis=3)
    tail_weighted = jnp.einsum(
        "rkgs,rskd->rkgd",
        tail_weights.astype(BF16),
        private_suffix_values,
        preferred_element_type=F32,
    )
    tail_out = (tail_weighted / tail_totals[..., None]).reshape(share, heads, size)
    tail_lse = (tail_high + jnp.log(tail_totals)).reshape(share, heads)
    own_out = take(prefix_out, first_own, share, 0)
    own_lse = take(prefix_lse, first_own, share, 0)
    own_out, own_lse = merge((own_out, own_lse), (tail_out, tail_lse))
    prefix_out = lax.dynamic_update_slice_in_dim(prefix_out, own_out, first_own, 0)
    prefix_lse = lax.dynamic_update_slice_in_dim(prefix_lse, own_lse, first_own, 0)

    half_heads = heads // 2
    state = (
        take(prefix_out, rep * half_heads, half_heads, 1),
        take(prefix_lse, rep * half_heads, half_heads, 1),
    )
    give = pack(
        take(prefix_out, (1 - rep) * half_heads, half_heads, 1),
        take(prefix_lse, (1 - rep) * half_heads, half_heads, 1),
    )
    out, lse = state
    lse = jnp.pad(lse, ((0, 0), (0, 128 - half_heads)))
    state = (out.reshape(rows, half_heads * size), lse)
    gots = [swap(give, "rep", 1)]
    for bits in plan:
        *state, send = merge_stage(state, gots, half_heads, size, False)
        gots = [swap(send, "seq", bit) for bit in bits]
    attended = merge_stage(state, gots, half_heads, size, True)

    other = swap(attended, "rep", 1)
    middle = weight_call(
        output_kernel,
        jax.ShapeDtypeStruct((rows, local), BF16),
        (w_output,),
        attended,
        other,
        steered,
    )

    shard_width = width // groups
    weights = (w_gate, w_up)
    gain = mlp_gain[None, :]
    if groups == 2 and seq_size >= 2:
        half = seq_size // 2
        near, far = [], []
        for s in range(seq_size):
            g = s // half
            near.append((2 * s + 1 - g, 2 * s + g))
            near.append((2 * s + g, 2 * (s ^ half) + g))
            far.append((2 * s + 1 - g, 2 * (s ^ half) + g))
        got = lax.ppermute(middle, ("seq", "head"), near)
        away = lax.ppermute(middle, ("seq", "head"), far)
        middle = arrive(lanes // 2, middle, got, away)
        stages = [("seq", bit) for bit in sorted(bits_of(half), reverse=True)] + [("rep", 1)]
        turns = [0]
        for axis, bit in stages:
            middle = join(middle, swap(middle, axis, bit))
            turns += [turn ^ (1 if axis == "rep" else 2 * bit) for turn in turns]

        def places(b):
            return (lane_index() % (lanes // 2)) ^ turns[b]

    else:
        for bit in bits_of(groups):
            middle = (middle.astype(F32) + swap(middle, "head", bit).astype(F32)).astype(BF16)
        middle = lax.all_gather(middle, LANES, axis=1, tiled=True)
        middle = take(middle, group * shard_width, shard_width, 1)

        def places(b):
            return b

    gate, up, tail, own_middle = wide_call(weights, places, local, share, middle, gain)

    ff_local = w_gate.shape[1]
    for bit in bits_of(groups):
        send = local_call(
            pack_kernel, jax.ShapeDtypeStruct((rows, 2 * ff_local + 128), BF16), gate, up, tail
        )
        got = swap(send, "head", bit)
        shapes = tuple(jax.ShapeDtypeStruct(x.shape, F32) for x in (gate, up, tail))
        gate, up, tail = local_call(combine_kernel, shapes, gate, up, tail, got)
    half_rows = rows // 2
    down, give = weight_call(
        functools.partial(down_kernel, lanes, width),
        (
            jax.ShapeDtypeStruct((half_rows, shard_width), F32),
            jax.ShapeDtypeStruct((half_rows, shard_width), BF16),
        ),
        (w_down,),
        gate,
        up,
        tail,
    )
    down = down + swap(give, "rep", 1).astype(F32)
    size_left = half_rows
    bits = list(bits_of(seq_size))
    seq = lax.axis_index("seq")
    for bit in bits[:-2]:
        size_left //= 2
        upper = (seq & bit) != 0
        low, high = down[:size_left], down[size_left:]
        got = swap(jnp.where(upper, low, high).astype(BF16), "seq", bit)
        down = jnp.where(upper, high, low) + got.astype(F32)
    unit = bits[-2]
    quarters = down.reshape(2, 2, share, shard_width)

    def quarter(place):
        one, two = place // unit % 2, place // (2 * unit) % 2
        part = lax.dynamic_index_in_dim(quarters, one, 0, keepdims=False)
        return lax.dynamic_index_in_dim(part, two, 0, keepdims=False)

    down = quarter(seq)
    gots = [
        swap(quarter(seq ^ bit).astype(BF16), "seq", bit)
        for bit in (unit, 2 * unit, 3 * unit)
    ]
    for got in gots:
        down = down + got.astype(F32)
    return (own_middle + down).astype(BF16)


def solution(mesh):
    return jax.shard_map(
        shards,
        mesh=mesh,
        in_specs=(
            P(("parts", "head"), ("seq", "rep")),
            P(("parts", "head"), None),
            P(None, ("seq", "rep")),
            P(("seq", "rep")),
            P(),
            P(("seq", "rep"), "head"),
            P("head", ("seq", "rep")),
            P("head", ("seq", "rep")),
            P("head", ("seq", "rep")),
            P(("seq", "rep"), "head"),
            P(("parts", "seq", "rep"), "head", None),
            P(("parts", "seq", "rep"), "head", None),
            P(("parts", "seq", "rep"), None, "head", None),
            P(("parts", "seq", "rep"), None, "head", None),
            P("parts"),
        ),
        out_specs=P(("parts", "seq", "rep"), "head"),
        check_vma=False,
    )
```

```python
import functools
import math

import jax
import jax.numpy as jnp
from jax import lax
from jax.experimental import pallas as pl
from jax.experimental.pallas import tpu as pltpu
from jax.sharding import PartitionSpec as P


QUERY_HEADS = 64
KEY_VALUE_HEADS = 8
EPSILON = 1e-05
ROPE_BASE = 500000.0
LANES = ("seq", "rep")
ARRIVE_WORK, JOIN_WORK = 3_000_000_000, 1_000_000_000
F32 = jnp.float32
BF16 = jnp.bfloat16


def swap(x, axis, bit):
    size = lax.axis_size(axis)
    return lax.ppermute(x, axis, [(i, i ^ bit) for i in range(size)])


def bits_of(size):
    bit = 1
    while bit < size:
        yield bit
        bit *= 2


def lane_index():
    return lax.axis_index("seq") * lax.axis_size("rep") + lax.axis_index("rep")


def take(x, start, size, axis):
    return lax.dynamic_slice_in_dim(x, start, size, axis)


def in_order(flag, mine, other, axis):
    first = jnp.where(flag, other, mine)
    second = jnp.where(flag, mine, other)
    return jnp.concatenate([first, second], axis=axis)


def split_parts(value, count):
    parts = []
    for _ in range(count):
        head = lax.reduce_precision(value, 8, 7)
        parts.append(head)
        value = value - head
    return parts


def local_call(body, outs, *args, flops=3_000_000_000):
    return pl.pallas_call(
        body,
        out_shape=outs,
        in_specs=[pl.BlockSpec(memory_space=pltpu.VMEM)] * len(args),
        cost_estimate=pl.CostEstimate(flops=flops, bytes_accessed=0, transcendentals=0),
        compiler_params=pltpu.CompilerParams(vmem_limit_bytes=4 << 20),
    )(*args)


def add_kernel(total_ref, *refs):
    *got_refs, next_ref, send_ref = refs
    total = total_ref[...]
    for got_ref in got_refs:
        total = total + got_ref[...].astype(F32)
    next_ref[...] = total
    send_ref[...] = total.astype(BF16)


def add_stage(total, gots):
    shapes = (
        jax.ShapeDtypeStruct(total.shape, F32),
        jax.ShapeDtypeStruct(total.shape, BF16),
    )
    return local_call(add_kernel, shapes, total, *gots)


def rope_kernel(width, total_ref, cosine_ref, sine_ref, *refs):
    *got_refs, out_ref = refs
    total = total_ref[...]
    for got_ref in got_refs:
        total = total + got_ref[...].astype(F32)
    wide = out_ref.shape[1]
    squares = jnp.sum(total[:, wide:], axis=1, keepdims=True)
    inverse = lax.rsqrt(squares / width + EPSILON)
    cosine, sine = cosine_ref[...], sine_ref[...]
    size = cosine.shape[1]
    for first in range(0, wide, size):
        head = total[:, first : first + size] * inverse
        turned = head * cosine + pltpu.roll(head, size // 2, 1) * sine
        out_ref[:, first : first + size] = turned.astype(BF16)


def arrive_kernel(half_lanes, mine_ref, near_ref, far_ref, out_ref):
    home = lane_index() // half_lanes == lax.axis_index("head")
    other = jnp.where(home, mine_ref[...], far_ref[...])
    out_ref[...] = (near_ref[...].astype(F32) + other.astype(F32)).astype(BF16)


def arrive(half_lanes, mine, near, far):
    return local_call(
        functools.partial(arrive_kernel, half_lanes),
        jax.ShapeDtypeStruct(mine.shape, BF16),
        mine,
        near,
        far,
        flops=ARRIVE_WORK,
    )


def join_kernel(one_ref, two_ref, out_ref):
    cut = one_ref.shape[1]
    out_ref[:, :cut] = one_ref[...]
    out_ref[:, cut:] = two_ref[...]


def join(one, two):
    shape = (one.shape[0], one.shape[1] + two.shape[1])
    return local_call(join_kernel, jax.ShapeDtypeStruct(shape, BF16), one, two, flops=JOIN_WORK)


def parts_of(value, heads):
    lane = lax.broadcasted_iota(jnp.int32, value.shape, 1)
    value = jnp.where(lane < heads, value, 0.0)
    packed = jnp.zeros_like(value)
    for i in range(3):
        head = value.astype(BF16).astype(F32)
        packed = packed + (pltpu.roll(head, i * heads, 1) if i else head)
        value = value - head
    return packed


def joined(packed, heads):
    lanes = packed.shape[1]
    value = packed
    for i in range(1, 3):
        value = value + pltpu.roll(packed, lanes - i * heads, 1)
    return value


def merge_kernel(heads, size, last, out_ref, lse_ref, *refs):
    count = len(refs) - (1 if last else 3)
    got_refs, refs = refs[:count], refs[count:]
    wide = heads * size
    lses = [lse_ref[...]] + [joined(ref[:, wide:].astype(F32), heads) for ref in got_refs]
    high = functools.reduce(jnp.maximum, lses)
    weights = [jnp.exp(lse - high) for lse in lses]
    total = functools.reduce(jnp.add, weights)
    shares = [weight / total for weight in weights]
    for h in range(heads):
        cols = slice(h * size, (h + 1) * size)
        merged = shares[0][:, h : h + 1] * out_ref[:, cols]
        for share, ref in zip(shares[1:], got_refs):
            merged = merged + share[:, h : h + 1] * ref[:, cols].astype(F32)
        if last:
            refs[0][:, cols] = merged.astype(BF16)
        else:
            refs[0][:, cols] = merged
            refs[2][:, cols] = merged.astype(BF16)
    if not last:
        lse = high + jnp.log(total)
        refs[1][...] = lse
        refs[2][:, wide:] = parts_of(lse, heads).astype(BF16)


def merge_stage(state, gots, heads, size, last):
    out, lse = state
    rows = out.shape[0]
    wide = heads * size
    if last:
        outs = jax.ShapeDtypeStruct((rows, wide), BF16)
    else:
        outs = (
            jax.ShapeDtypeStruct((rows, wide), F32),
            jax.ShapeDtypeStruct(lse.shape, F32),
            jax.ShapeDtypeStruct((rows, wide + lse.shape[1]), BF16),
        )
    body = functools.partial(merge_kernel, heads, size, last)
    return local_call(body, outs, out, lse, *gots)


def rope_tables(positions, width):
    half = width // 2
    exponent = jnp.arange(half, dtype=F32) * (2.0 / width)
    frequency = jnp.exp(-math.log(ROPE_BASE) * exponent)
    angles = positions.astype(F32)[:, None] * frequency[None, :]
    cosine, sine = jnp.cos(angles), jnp.sin(angles)
    return jnp.concatenate([cosine, cosine], axis=1), jnp.concatenate([-sine, sine], axis=1)


def exchanges(size):
    bits = list(bits_of(size))
    if len(bits) < 2:
        return [[bit] for bit in bits]
    low, high = bits[-2:]
    return [[bit] for bit in bits[:-2]] + [[low, high, low | high]]


def merge(one, two):
    out_one, lse_one = one
    out_two, lse_two = two
    high = jnp.maximum(lse_one, lse_two)
    w_one = jnp.exp(lse_one - high)
    w_two = jnp.exp(lse_two - high)
    total = w_one + w_two
    out = out_one * (w_one / total)[..., None] + out_two * (w_two / total)[..., None]
    return out, high + jnp.log(total)


def pack(out, lse):
    rows, heads, size = out.shape
    parts = jnp.concatenate(split_parts(lse, 3), axis=1)
    pad = -parts.shape[1] % 128
    parts = jnp.pad(parts, ((0, 0), (0, pad)))
    return jnp.concatenate([out.reshape(rows, heads * size), parts], axis=1).astype(BF16)


def steps_of(size, most):
    step = min(size, most)
    while size % step or (step < size and step % 128):
        step -= 1
    return step


def weight_call(body, outs, weights, *args):
    count = len(weights)
    total = sum(weight.size * weight.dtype.itemsize for weight in weights)

    def kernel(*refs):
        body(refs[:count], *refs[count:])

    return pl.pallas_call(
        kernel,
        out_shape=outs,
        in_specs=[pl.BlockSpec(memory_space=pltpu.VMEM)] * (count + len(args)),
        cost_estimate=pl.CostEstimate(flops=0, bytes_accessed=total, transcendentals=0),
        compiler_params=pltpu.CompilerParams(vmem_limit_bytes=total + (4 << 20)),
    )(*weights, *args)


def seal_kernel(lanes, gained_ref, squares_ref, out_ref):
    local = gained_ref.shape[1]
    out_ref[:, :local] = gained_ref[...]
    squares = squares_ref[...]
    high = squares.astype(BF16).astype(F32)
    low = squares - high
    slot = lax.broadcasted_iota(jnp.int32, (squares.shape[0], out_ref.shape[1] - local), 1)
    lane = lane_index()
    tail = jnp.where(slot == lane, high, jnp.where(slot == lane + lanes, low, 0.0))
    out_ref[:, local:] = tail.astype(BF16)


def query_kernel(local, weights, *refs):
    *x_refs, mine_ref, give_ref = refs
    (weight,) = weights
    x = x_refs[0][...]
    if len(x_refs) == 2:
        other = x_refs[1][...]
        second = lax.axis_index("head") == 1
        x = jnp.concatenate([jnp.where(second, other, x), jnp.where(second, x, other)], axis=0)
    half = weight.shape[1] // 2
    upper = lax.axis_index("rep") == 1
    step = steps_of(half, 1024)
    for c in range(0, half, step):
        low = jnp.dot(x[:, :local], weight[:, c : c + step], preferred_element_type=F32)
        high = jnp.dot(
            x[:, :local], weight[:, half + c : half + c + step], preferred_element_type=F32
        )
        mine_ref[:, c : c + step] = jnp.where(upper, high, low)
        give_ref[:, c : c + step] = jnp.where(upper, low, high).astype(BF16)
    mine_ref[:, half:] = x[:, local:].astype(F32)
    give_ref[:, half:] = x[:, local:]


def output_kernel(weights, mine_ref, other_ref, steered_ref, out_ref):
    (weight,) = weights
    half = weight.shape[0] // 2
    step = steps_of(half, 1024)
    total = jnp.zeros(out_ref.shape, F32)
    upper = lax.axis_index("rep") == 1
    for k in range(0, half, step):
        cols = slice(k, k + step)
        mine, other = mine_ref[:, cols], other_ref[:, cols]
        low, high = jnp.where(upper, other, mine), jnp.where(upper, mine, other)
        total += jnp.dot(low, weight[k : k + step, :], preferred_element_type=F32)
        total += jnp.dot(high, weight[half + k : half + k + step, :], preferred_element_type=F32)
    block = steered_ref.shape[0]
    for g in range(out_ref.shape[0] // block):
        rows = slice(g * block, (g + 1) * block)
        own = jnp.where(lax.axis_index("head") == g, steered_ref[...], 0.0)
        out_ref[rows, :] = (total[rows] + own).astype(BF16)


def wide_kernel(local, places, weights, x_ref, gain_ref, *refs):
    gate, up, tail_ref, own_ref = refs[-4:]
    before = refs[:-4]
    wide = x_ref.shape[1]
    x = x_ref[...].astype(F32)
    squares = jnp.sum(x * x, axis=1, keepdims=True)
    lane = lax.broadcasted_iota(jnp.int32, tail_ref.shape, 1)
    tail_ref[...] = jnp.where(lane == 0, squares, 0.0)
    own_ref[...] = before[3][...] if before else jnp.zeros(own_ref.shape, F32)
    sums = [None] * len(weights)
    row = lax.broadcasted_iota(jnp.int32, (x.shape[0], local), 0)
    for b in range(wide // local):
        place = places(b)
        start = pl.multiple_of(place * local, local)
        whole = lax.axis_index("head") * weights[0].shape[0] + place * local
        scale = gain_ref[:, pl.ds(pl.multiple_of(whole, local), local)]
        block = x[:, b * local : (b + 1) * local]
        part = (block * scale).astype(BF16)
        for i in range(own_ref.shape[0]):
            own = jnp.where(row == lane_index() * own_ref.shape[0] + i, block, 0.0)
            own_ref[i : i + 1, pl.ds(start, local)] = jnp.sum(own, axis=0, keepdims=True)
        for n, weight in enumerate(weights):
            got = jnp.dot(part, weight[pl.ds(start, local), :], preferred_element_type=F32)
            sums[n] = got if sums[n] is None else sums[n] + got
    gate[...] = sums[0] + before[0][...] if before else sums[0]
    up[...] = sums[1] + before[1][...] if before else sums[1]
    if before:
        tail_ref[...] += before[2][...]


def wide_call(weights, places, local, share, x, gain, before=()):
    rows = x.shape[0]
    outs = [jax.ShapeDtypeStruct((rows, weights[0].shape[1]), F32)] * 2
    outs.append(jax.ShapeDtypeStruct((rows, 128), F32))
    outs.append(jax.ShapeDtypeStruct((share, weights[0].shape[0]), F32))
    body = functools.partial(wide_kernel, local, places)
    return weight_call(body, tuple(outs), weights, x, gain, *before)


def pack_kernel(gate_ref, up_ref, tail_ref, out_ref):
    cut = gate_ref.shape[1]
    out_ref[:, :cut] = gate_ref[...].astype(BF16)
    out_ref[:, cut : 2 * cut] = up_ref[...].astype(BF16)
    out_ref[:, 2 * cut :] = parts_of(tail_ref[...], 1).astype(BF16)


def combine_kernel(gate_ref, up_ref, tail_ref, got_ref, gate_out, up_out, tail_out):
    cut = gate_ref.shape[1]
    gate_out[...] = gate_ref[...] + got_ref[:, :cut].astype(F32)
    up_out[...] = up_ref[...] + got_ref[:, cut : 2 * cut].astype(F32)
    tail_out[...] = tail_ref[...] + joined(got_ref[:, 2 * cut :].astype(F32), 1)


def down_kernel(lanes, width, weights, gate_ref, up_ref, tail_ref, mine_ref, give_ref):
    (weight,) = weights
    rows, _ = gate_ref.shape
    inverse = lax.rsqrt(tail_ref[:, :1] / width + EPSILON)
    gate = gate_ref[...] * inverse
    up = up_ref[...] * inverse
    hidden = (gate / (1.0 + jnp.exp(-gate)) * up).astype(BF16)
    share = rows // lanes
    row = lax.broadcasted_iota(jnp.int32, (rows, rows), 0)
    source = lax.broadcasted_iota(jnp.int32, (rows, rows), 1)
    left, turned = row // share, jnp.zeros_like(row)
    for _ in range(lanes.bit_length() - 1):
        turned = turned * 2 + left % 2
        left = left // 2
    turned = turned * share + row % share
    order = (turned == source).astype(F32).astype(BF16)
    hidden = jnp.dot(order, hidden, preferred_element_type=F32).astype(BF16)
    half = rows // 2
    upper = lax.axis_index("rep") == 1
    step = steps_of(weight.shape[1], 1024)
    for c in range(0, weight.shape[1], step):
        cols = slice(c, c + step)
        block = jnp.dot(hidden, weight[:, cols], preferred_element_type=F32)
        low, high = block[:half], block[half:]
        mine_ref[:, cols] = jnp.where(upper, high, low)
        give_ref[:, cols] = jnp.where(upper, low, high).astype(BF16)


def shards(
    residual,
    coefficients,
    directions,
    attn_gain,
    mlp_gain,
    w_query,
    w_output,
    w_gate,
    w_up,
    w_down,
    prefix_keys,
    prompt_value_rows,
    private_suffix_keys,
    private_suffix_values,
    suffix_lengths,
):
    lanes = lax.axis_size(LANES)
    lane = lax.axis_index(LANES)
    rep = lax.axis_index("rep")
    seq_size = lax.axis_size("seq")
    groups = lax.axis_size("head")
    group = lax.axis_index("head")
    block_rows = residual.shape[0]
    rows = block_rows * groups
    share = rows // lanes
    first_own = lane * share
    width = w_gate.shape[0] * groups
    prompt_length = prefix_keys.shape[0] * lanes
    kv_local, size = prefix_keys.shape[1:]
    heads_per_group = QUERY_HEADS // KEY_VALUE_HEADS
    heads = kv_local * heads_per_group
    suffix_tokens = private_suffix_keys.shape[1]

    local = residual.shape[1]
    slots = 2 * lanes + (-2 * lanes % 128)
    steered = residual.astype(F32) + jnp.dot(
        coefficients, directions, precision=lax.Precision.HIGHEST
    )
    squares = jnp.sum(steered * steered, axis=1, keepdims=True)
    gained = local_call(
        functools.partial(seal_kernel, lanes),
        jax.ShapeDtypeStruct((block_rows, local + slots), BF16),
        (steered * attn_gain[None, :]).astype(BF16),
        squares,
    )
    if groups == 2:
        gained = (gained, swap(gained, "head", 1))
    else:
        gained = (lax.all_gather(gained, "head", axis=0, tiled=True),)

    columns = w_query.shape[1] // 2
    wide = columns + slots
    mine, give = weight_call(
        functools.partial(query_kernel, local),
        (jax.ShapeDtypeStruct((rows, wide), F32), jax.ShapeDtypeStruct((rows, wide), BF16)),
        (w_query,),
        *gained,
    )
    total = mine + swap(give, "rep", 1).astype(F32)
    send = total.astype(BF16)
    cosine, sine = rope_tables(prompt_length + suffix_lengths - 1, size)
    plan = exchanges(seq_size)
    for bits in plan[:-1]:
        total, send = add_stage(total, [swap(send, "seq", bit) for bit in bits])
    half_queries = local_call(
        functools.partial(rope_kernel, width),
        jax.ShapeDtypeStruct((rows, columns), BF16),
        total,
        cosine,
        sine,
        *[swap(send, "seq", bit) for bit in plan[-1]],
    )
    queries = in_order(rep == 1, half_queries, swap(half_queries, "rep", 1), 1)
    queries = queries.reshape(rows, kv_local, heads_per_group, size)

    scale = 1.0 / math.sqrt(size)
    scores = (
        jnp.einsum("rkgd,pkd->rkgp", queries, prefix_keys, preferred_element_type=F32) * scale
    )
    highest = jnp.max(scores, axis=3)
    weights = jnp.exp(scores - highest[..., None])
    totals = jnp.sum(weights, axis=3)
    weighted = jnp.einsum(
        "rkgp,pkd->rkgd", weights.astype(BF16), prompt_value_rows, preferred_element_type=F32
    )
    prefix_out = (weighted / totals[..., None]).reshape(rows, heads, size)
    prefix_lse = (highest + jnp.log(totals)).reshape(rows, heads)
    own_queries = take(queries, first_own, share, 0)
    own_lengths = take(suffix_lengths, first_own, share, 0)
    live = (jnp.arange(suffix_tokens)[None, :] < own_lengths[:, None])[:, None, None, :]
    tail_scores = (
        jnp.einsum(
            "rkgd,rskd->rkgs", own_queries, private_suffix_keys, preferred_element_type=F32
        )
        * scale
    )
    tail_scores = jnp.where(live, tail_scores, -jnp.inf)
    tail_high = jnp.max(tail_scores, axis=3)
    tail_weights = jnp.where(live, jnp.exp(tail_scores - tail_high[..., None]), 0.0)
    tail_totals = jnp.sum(tail_weights, axis=3)
    tail_weighted = jnp.einsum(
        "rkgs,rskd->rkgd",
        tail_weights.astype(BF16),
        private_suffix_values,
        preferred_element_type=F32,
    )
    tail_out = (tail_weighted / tail_totals[..., None]).reshape(share, heads, size)
    tail_lse = (tail_high + jnp.log(tail_totals)).reshape(share, heads)
    own_out = take(prefix_out, first_own, share, 0)
    own_lse = take(prefix_lse, first_own, share, 0)
    own_out, own_lse = merge((own_out, own_lse), (tail_out, tail_lse))
    prefix_out = lax.dynamic_update_slice_in_dim(prefix_out, own_out, first_own, 0)
    prefix_lse = lax.dynamic_update_slice_in_dim(prefix_lse, own_lse, first_own, 0)

    half_heads = heads // 2
    state = (
        take(prefix_out, rep * half_heads, half_heads, 1),
        take(prefix_lse, rep * half_heads, half_heads, 1),
    )
    give = pack(
        take(prefix_out, (1 - rep) * half_heads, half_heads, 1),
        take(prefix_lse, (1 - rep) * half_heads, half_heads, 1),
    )
    out, lse = state
    lse = jnp.pad(lse, ((0, 0), (0, 128 - half_heads)))
    state = (out.reshape(rows, half_heads * size), lse)
    gots = [swap(give, "rep", 1)]
    for bits in plan:
        *state, send = merge_stage(state, gots, half_heads, size, False)
        gots = [swap(send, "seq", bit) for bit in bits]
    attended = merge_stage(state, gots, half_heads, size, True)

    other = swap(attended, "rep", 1)
    middle = weight_call(
        output_kernel,
        jax.ShapeDtypeStruct((rows, local), BF16),
        (w_output,),
        attended,
        other,
        steered,
    )

    shard_width = width // groups
    weights = (w_gate, w_up)
    gain = mlp_gain[None, :]
    if groups == 2 and seq_size >= 2:
        half = seq_size // 2
        near, far = [], []
        for s in range(seq_size):
            g = s // half
            near.append((2 * s + 1 - g, 2 * s + g))
            near.append((2 * s + g, 2 * (s ^ half) + g))
            far.append((2 * s + 1 - g, 2 * (s ^ half) + g))
        got = lax.ppermute(middle, ("seq", "head"), near)
        away = lax.ppermute(middle, ("seq", "head"), far)
        middle = arrive(lanes // 2, middle, got, away)
        stages = [("seq", bit) for bit in sorted(bits_of(half), reverse=True)] + [("rep", 1)]
        turns = [0]
        for axis, bit in stages[:-1]:
            middle = join(middle, swap(middle, axis, bit))
            turns += [turn ^ (2 * bit) for turn in turns]

        def places(turn, b):
            return (lane_index() % (lanes // 2)) ^ turns[b] ^ turn

        mine = functools.partial(places, 0)
        middle, rest = lax.optimization_barrier(
            (swap(middle, "rep", 1), wide_call(weights, mine, local, share, middle, gain))
        )
        places = functools.partial(places, 1)
    else:
        for bit in bits_of(groups):
            middle = (middle.astype(F32) + swap(middle, "head", bit).astype(F32)).astype(BF16)
        middle = lax.all_gather(middle, LANES, axis=1, tiled=True)
        middle = take(middle, group * shard_width, shard_width, 1)

        def places(b):
            return b

        rest = ()

    gate, up, tail, own_middle = wide_call(
        weights, places, local, share, middle, gain, rest
    )

    ff_local = w_gate.shape[1]
    for bit in bits_of(groups):
        send = local_call(
            pack_kernel, jax.ShapeDtypeStruct((rows, 2 * ff_local + 128), BF16), gate, up, tail
        )
        got = swap(send, "head", bit)
        shapes = tuple(jax.ShapeDtypeStruct(x.shape, F32) for x in (gate, up, tail))
        gate, up, tail = local_call(combine_kernel, shapes, gate, up, tail, got)
    half_rows = rows // 2
    down, give = weight_call(
        functools.partial(down_kernel, lanes, width),
        (
            jax.ShapeDtypeStruct((half_rows, shard_width), F32),
            jax.ShapeDtypeStruct((half_rows, shard_width), BF16),
        ),
        (w_down,),
        gate,
        up,
        tail,
    )
    down = down + swap(give, "rep", 1).astype(F32)
    size_left = half_rows
    bits = list(bits_of(seq_size))
    seq = lax.axis_index("seq")
    for bit in bits[:-2]:
        size_left //= 2
        upper = (seq & bit) != 0
        low, high = down[:size_left], down[size_left:]
        got = swap(jnp.where(upper, low, high).astype(BF16), "seq", bit)
        down = jnp.where(upper, high, low) + got.astype(F32)
    unit = bits[-2]
    quarters = down.reshape(2, 2, share, shard_width)

    def quarter(place):
        one, two = place // unit % 2, place // (2 * unit) % 2
        part = lax.dynamic_index_in_dim(quarters, one, 0, keepdims=False)
        return lax.dynamic_index_in_dim(part, two, 0, keepdims=False)

    down = quarter(seq)
    gots = [
        swap(quarter(seq ^ bit).astype(BF16), "seq", bit)
        for bit in (unit, 2 * unit, 3 * unit)
    ]
    for got in gots:
        down = down + got.astype(F32)
    return (own_middle + down).astype(BF16)


def solution(mesh):
    return jax.shard_map(
        shards,
        mesh=mesh,
        in_specs=(
            P(("parts", "head"), ("seq", "rep")),
            P(("parts", "head"), None),
            P(None, ("seq", "rep")),
            P(("seq", "rep")),
            P(),
            P(("seq", "rep"), "head"),
            P("head", ("seq", "rep")),
            P("head", ("seq", "rep")),
            P("head", ("seq", "rep")),
            P(("seq", "rep"), "head"),
            P(("parts", "seq", "rep"), "head", None),
            P(("parts", "seq", "rep"), "head", None),
            P(("parts", "seq", "rep"), None, "head", None),
            P(("parts", "seq", "rep"), None, "head", None),
            P("parts"),
        ),
        out_specs=P(("parts", "seq", "rep"), "head"),
        check_vma=False,
    )
```
